256 devices in a mesh: atom: 32 (over y_lo, z, core), band: 8 (over y_hi, x).
Axes of the slice: x: 4, y: 4 (y_hi: 2, y_lo: 2; y = y_hi * 2 + y_lo), z: 8, core: 2. Of those that a mesh axis runs over, the one named last changes fastest.
Arguments:
- wave_rows: bfloat16 [512, 65536], P('atom', 'band'), may hold values from -6 to 6
- projectors: bfloat16 [4096, 65536], P('atom', 'band'), may hold values from -0.0234375 to 0.0234375
- dij_table: float32 [16, 8, 8], replicated, may hold values from -6 to 6
- dij_index: int32 [512], P('atom'), may hold values from 0 to 15
- proj_count: int32 [512], P('atom'), may hold values from 1 to 8
Outputs:
- nonlocal_rows: bfloat16 [512, 65536], P('atom', 'band')
The draws below stay inside these ranges and needn't reach their ends.
All inputs are finite; a program needn't handle non-finite values.
Results may differ from the reference program's by a relative error of at most 0.0049.
Values may be sent and summed in bfloat16 or wider, within the bound.
A program may use at most 128 MiB of HBM per device.

```python
import jax
import jax.numpy as jnp
from jax import lax

G = 65536
PROJ = 8
KINDS = 16
ATOMS = 512
BANDS = 512


def touch_ends(entries, rng, smallest, high):
    extent = entries.shape
    index_at = [jax.random.randint(jax.random.fold_in(rng, axis), (), 0, extent[axis]) for axis in range(len(extent))]
    entries = entries.at[tuple(index_at)].set(smallest)
    longest = extent.index(max(extent))
    index_at[longest] = (index_at[longest] + 1) % extent[longest]
    return entries.at[tuple(index_at)].set(high)


def block_levels(own_key, dims, shards, smallest, high):
    loudness, own = 1.0, jax.random.fold_in(own_key, 6)
    for dim, parts in shards:
        heights = jnp.exp(jax.random.uniform(jax.random.fold_in(own, dim), (parts,), jnp.float32, smallest / len(shards), high / len(shards)))
        loudness = loudness * jnp.repeat(heights, dims[dim] // parts).reshape([-1 if axis == dim else 1 for axis in range(len(dims))])
    return loudness


def scatter_about(key, dims, width, limit, pieces=(), held_as=jnp.bfloat16):
    values = jax.random.normal(key, dims, jnp.float32) * width
    if len(pieces) > 0:
        values = block_levels(key, dims, pieces, -0.22, 0.18) * values
    return jnp.clip(values, min=-limit, max=limit).astype(held_as)


def setup_inputs(seed: int = 0) -> dict:
    key_list = jax.random.split(jax.random.key(seed), 6)
    return {
        "wave_rows": scatter_about(key_list[0], (BANDS, G), 1.0, 6.0, ((0, 32), (1, 8))),
        "projectors": scatter_about(key_list[1], (ATOMS * PROJ, G), G ** -0.5, 0.0234375, ((0, 32), (1, 8))),
        "dij_table": scatter_about(key_list[2], (KINDS, PROJ, PROJ), 1.0, 6.0, (), jnp.float32),
        "dij_index": touch_ends(jax.random.randint(key_list[3], (ATOMS,), 0, KINDS), jax.random.fold_in(key_list[3], 1), 0, KINDS - 1).astype(jnp.int32),
        "proj_count": touch_ends(jax.random.randint(key_list[4], (ATOMS,), 1, PROJ + 1), jax.random.fold_in(key_list[4], 1), 1, PROJ).astype(jnp.int32),
    }


def reference(wave_rows, projectors, dij_table, dij_index, proj_count):
    intersections = jnp.dot(wave_rows, projectors.T, preferred_element_type=jnp.float32)
    kind_onehot = (dij_index[:, None] == jnp.arange(KINDS, dtype=jnp.int32)[None, :]).astype(jnp.float32)
    blocks = jnp.dot(kind_onehot, dij_table.reshape(KINDS, PROJ * PROJ), precision=lax.Precision.HIGHEST).reshape(ATOMS, PROJ, PROJ)
    active = (jnp.arange(PROJ, dtype=jnp.int32)[None, :] < proj_count[:, None]).astype(jnp.float32)
    blocks = blocks * active[:, :, None] * active[:, None, :]
    weighted = jnp.einsum("baj,aij->bai", intersections.reshape(BANDS, ATOMS, PROJ), blocks, precision=lax.Precision.HIGHEST)
    weighted = weighted.reshape(BANDS, ATOMS * PROJ).astype(jnp.bfloat16)
    return jnp.dot(weighted, projectors, preferred_element_type=jnp.float32).astype(jnp.bfloat16)
```

```python
import functools

import jax
import jax.numpy as jnp
from jax import lax
from jax.experimental import pallas as pl
from jax.experimental.pallas import tpu as pltpu
from jax.sharding import PartitionSpec as P

MESH = pl.DeviceIdType.MESH
F32 = jnp.float32
BF16 = jnp.bfloat16
Z = 8
SIDE = 4
PLANE = SIDE * SIDE
PIECES = 4
UP, DOWN = 0, 1
STEPS = {(0, UP): 4, (0, DOWN): 3, (1, UP): 3, (1, DOWN): 4}
RING = [(t, k, d) for t in range(4) for k in (0, 1) for d in (UP, DOWN) if t < STEPS[k, d]]


def kernel(
    wave_ref, proj_ref, coef_ref, out_ref,
    bands, away, proj, coefs, part, parts, weighted, result, sent, came, final, mix,
    ring_send, ring_recv, y_send, y_recv, c_send, c_recv, piece_send, piece_recv, pass_send, pass_recv,
    part_send, part_recv, wt_send, wt_recv, sum_send, sum_recv, local_sem,
):
    rows, half = away.shape
    count = coef_ref.shape[1]
    atom, band = lax.axis_index("atom"), lax.axis_index("band")
    y_lo, z, core = atom // (2 * Z), (atom // 2) % Z, atom % 2
    y_hi, x = band // SIDE, band % SIDE
    y = y_hi * 2 + y_lo
    me = y * SIDE + x
    slot = y_lo * 2 + core

    def at(lo, zz, cc, hi=y_hi, xx=x):
        return (lo * (2 * Z) + zz * 2 + cc, hi * SIDE + xx)

    mate = at(y_lo, z, 1 - core)
    across = at(1 - y_lo, z, core)
    corner = at(1 - y_lo, z, 1 - core)
    z_next = (at(y_lo, (z + 1) % Z, core), at(y_lo, (z + Z - 1) % Z, core))
    shifts = [(dy, dx) for dy in range(SIDE) for dx in range(SIDE) if dy or dx]

    def plane(dy, dx):
        yy, xx = (y + dy) % SIDE, (x + dx) % SIDE
        return yy * SIDE + xx, at(yy % 2, z, core, yy // 2, xx)

    def remote(src, dst, send, recv, to):
        return pltpu.make_async_remote_copy(
            src_ref=src, dst_ref=dst, send_sem=send, recv_sem=recv, device_id=to, device_id_type=MESH
        )

    mine = pl.ds(pl.multiple_of(y_lo * half, half), half)
    theirs = pl.ds(pl.multiple_of((1 - y_lo) * half, half), half)

    own_bands = pltpu.make_async_copy(wave_ref.at[:, mine], bands.at[z * 2 + y_lo], local_sem.at[0])
    away_bands = pltpu.make_async_copy(wave_ref.at[:, theirs], away, local_sem.at[1])
    own_proj = pltpu.make_async_copy(proj_ref.at[:, mine], proj.at[slot], local_sem.at[2])
    own_coefs = pltpu.make_async_copy(coef_ref, coefs.at[slot], local_sem.at[3])
    for copy in (own_bands, away_bands, own_coefs, own_proj):
        copy.start()

    barrier = pltpu.get_barrier_semaphore()
    greet = [mate, corner, *z_next] + [plane(*s)[1] for s in shifts]
    for to in greet:
        pl.semaphore_signal(barrier, inc=1, device_id=to, device_id_type=MESH)
    pl.semaphore_wait(barrier, len(greet))

    started = []

    def go(copy):
        copy.start()
        started.append(copy)

    def ring_copy(k, d, t):
        source = (z + Z - t) % Z if d == UP else (z + t) % Z
        index = source * 2 + (y_lo if k == 0 else 1 - y_lo)
        return remote(bands.at[index], bands.at[index], ring_send.at[k, d, t], ring_recv.at[k, d, t], z_next[d])

    away_bands.wait()
    y_bands = remote(away, bands.at[z * 2 + y_lo], y_send.at[0], y_recv.at[0], across)
    go(y_bands)
    own_bands.wait()
    for d in (UP, DOWN):
        go(ring_copy(0, d, 0))
    own_coefs.wait()
    coef_copies = [
        remote(coefs.at[slot], coefs.at[slot], c_send.at[i], c_recv.at[i], to) for i, to in enumerate((mate, across, corner))
    ]
    for copy in coef_copies:
        go(copy)
    size = count // PIECES
    pieces = [
        remote(
            proj_ref.at[pl.ds(i * size, size), theirs],
            proj.at[slot, pl.ds(i * size, size), :],
            piece_send.at[i], piece_recv.at[i], across,
        )
        for i in range(PIECES)
    ]
    for copy in pieces:
        go(copy)
    own_proj.wait()
    to_mate = remote(proj.at[slot], proj.at[slot], y_send.at[1], y_recv.at[1], mate)
    go(to_mate)

    y_bands.wait_recv()
    for d in (UP, DOWN):
        go(ring_copy(1, d, 0))
    far = (1 - y_lo) * 2 + core
    passed = []
    for t in range(4):
        for k in (0, 1):
            for d in (UP, DOWN):
                if t < STEPS[k, d]:
                    ring_copy(k, d, t).wait_recv()
                    if t + 1 < STEPS[k, d]:
                        go(ring_copy(k, d, t + 1))
        pieces[t].wait_recv()
        block = proj.at[far, pl.ds(t * size, size), :]
        passing = remote(block, block, pass_send.at[t], pass_recv.at[t], mate)
        go(passing)
        passed.append(passing)

    for copy in coef_copies:
        copy.wait_recv()
    same = lax.broadcasted_iota(jnp.int32, (128, 128), 0) // 8 == lax.broadcasted_iota(jnp.int32, (128, 128), 1) // 8
    for s in range(4):
        mix[s] = jnp.where(same, jnp.concatenate([coefs[s]] * 16, axis=0), 0.0)
    to_mate.wait_recv()
    for copy in passed:
        copy.wait_recv()

    every = PLANE * rows

    @pl.loop(0, 2)
    def _(n):
        value = lax.dot_general(
            bands[...].reshape(every, half),
            proj[pl.ds(n * 2, 2)].reshape(2 * count, half),
            (((1,), (1,)), ((), ())),
            preferred_element_type=F32,
        )
        part[:, :, pl.ds(pl.multiple_of(n * 2 * count, 2 * count), 2 * count)] = value.reshape(PLANE, rows, 2 * count)

    part_copies = []
    for i, s in enumerate(shifts):
        chunk, to = plane(*s)
        part_copies.append(remote(part.at[chunk], parts.at[i], part_send.at[i], part_recv.at[i], to))
        go(part_copies[-1])
    total = part[me]
    for i, copy in enumerate(part_copies):
        copy.wait_recv()
        total += parts[i]
    mixed = [
        jnp.dot(
            total[:, s * count : (s + 1) * count], mix[s], precision=lax.Precision.HIGHEST, preferred_element_type=F32
        )
        for s in range(4)
    ]
    weighted[me] = jnp.concatenate(mixed, axis=1).astype(BF16)
    wt_copies = []
    for i, s in enumerate(shifts):
        _, to = plane(*s)
        wt_copies.append(remote(weighted.at[me], weighted.at[me], wt_send.at[i], wt_recv.at[i], to))
        go(wt_copies[-1])
    for copy in wt_copies:
        copy.wait_recv()

    tile = 512

    @pl.loop(0, half // tile)
    def _(n):
        columns = pl.ds(pl.multiple_of(n * tile, tile), tile)
        value = jnp.dot(
            weighted[...].reshape(every, 4 * count),
            proj[:, :, columns].reshape(4 * count, tile),
            preferred_element_type=F32,
        )
        result[:, :, columns] = value.reshape(PLANE, rows, tile)

    width = half // 2

    def own_sum(owner, k):
        return result[pl.ds(owner * 2, 2), :, pl.ds(k * width, width)]

    def sum_copy(k, d, t):
        return remote(sent.at[k, d, t], came.at[k, d, t], sum_send.at[k, d, t], sum_recv.at[k, d, t], z_next[d])

    for t in range(5):
        for k in (0, 1):
            for d in (UP, DOWN):
                n = STEPS[k, d]
                if t < n:
                    owner = (z + (n - t)) % Z if d == UP else (z + Z - (n - t)) % Z
                    value = own_sum(owner, k)
                    if t > 0:
                        sum_copy(k, d, t - 1).wait_recv()
                        value += came[k, d, t - 1].astype(F32)
                    sent[k, d, t] = value.astype(BF16)
                    go(sum_copy(k, d, t))
    ends = []
    outs = []
    for k in (0, 1):
        value = own_sum(z, k)
        for d in (UP, DOWN):
            last = STEPS[k, d] - 1
            sum_copy(k, d, last).wait_recv()
            value += came[k, d, last].astype(F32)
        final[:, :, k * width : (k + 1) * width] = value.astype(BF16)
        columns = pl.ds(pl.multiple_of(y_lo * half + k * width, width), width)
        there = remote(
            final.at[1 - y_lo, :, pl.ds(k * width, width)], out_ref.at[:, columns], y_send.at[2 + k], y_recv.at[2 + k], across
        )
        go(there)
        ends.append(there)
        here = pltpu.make_async_copy(
            final.at[y_lo, :, pl.ds(k * width, width)], out_ref.at[:, columns], local_sem.at[4 + k]
        )
        here.start()
        outs.append(here)
    for copy in ends:
        copy.wait_recv()
    for copy in outs:
        copy.wait()
    for copy in started:
        copy.wait_send()


def shards(wave_rows, projectors, dij_table, dij_index, proj_count):
    rows, width = wave_rows.shape
    count = projectors.shape[0]
    half = width // 2
    kinds, per_atom, _ = dij_table.shape
    index = jnp.repeat(dij_index, per_atom)
    acting = jnp.repeat(proj_count, per_atom)
    place = jnp.arange(count, dtype=jnp.int32) % per_atom
    spread = jnp.tile(jnp.transpose(dij_table, (0, 2, 1)), (1, 1, count // per_atom))
    chosen = jnp.where(index[None, None, :] == jnp.arange(kinds, dtype=jnp.int32)[:, None, None], spread, 0.0)
    coefs = jnp.sum(chosen, axis=0)
    rows_on = jnp.arange(per_atom, dtype=jnp.int32)[:, None] < acting[None, :]
    coefs = jnp.where(rows_on & (place < acting)[None, :], coefs, 0.0)

    dma = pltpu.SemaphoreType.DMA
    others = PLANE - 1
    return pl.pallas_call(
        kernel,
        out_shape=jax.ShapeDtypeStruct((rows, width), BF16),
        in_specs=[pl.BlockSpec(memory_space=pl.ANY)] * 3,
        out_specs=pl.BlockSpec(memory_space=pl.ANY),
        scratch_shapes=[
            pltpu.VMEM((PLANE, rows, half), BF16),
            pltpu.VMEM((rows, half), BF16),
            pltpu.VMEM((4, count, half), BF16),
            pltpu.VMEM((4, per_atom, count), F32),
            pltpu.VMEM((PLANE, rows, 4 * count), F32),
            pltpu.VMEM((others, rows, 4 * count), F32),
            pltpu.VMEM((PLANE, rows, 4 * count), BF16),
            pltpu.VMEM((PLANE, rows, half), F32),
            pltpu.VMEM((2, 2, 4, 2, rows, half // 2), BF16),
            pltpu.VMEM((2, 2, 4, 2, rows, half // 2), BF16),
            pltpu.VMEM((2, rows, half), BF16),
            pltpu.VMEM((4, count, count), F32),
            dma((2, 2, 4)), dma((2, 2, 4)),
            dma((4,)), dma((4,)),
            dma((3,)), dma((3,)),
            dma((PIECES,)), dma((PIECES,)),
            dma((PIECES,)), dma((PIECES,)),
            dma((others,)), dma((others,)),
            dma((others,)), dma((others,)),
            dma((2, 2, 4)), dma((2, 2, 4)),
            dma((6,)),
        ],
        compiler_params=pltpu.CompilerParams(
            collective_id=0, has_side_effects=True, vmem_limit_bytes=48 * 1024 * 1024
        ),
        name="nonlocal_rows",
    )(wave_rows, projectors, coefs)


def solution(mesh):
    return jax.shard_map(
        shards,
        mesh=mesh,
        in_specs=(P("atom", "band"), P("atom", "band"), P(), P("atom"), P("atom")),
        out_specs=P("atom", "band"),
        check_vma=False,
    )
```

```python
import functools

import jax
import jax.numpy as jnp
from jax import lax
from jax.experimental import pallas as pl
from jax.experimental.pallas import tpu as pltpu
from jax.sharding import PartitionSpec as P

MESH = pl.DeviceIdType.MESH
F32 = jnp.float32
BF16 = jnp.bfloat16
scope = jax.named_scope
Z = 8
SIDE = 4
PLANE = SIDE * SIDE
PIECES = 4
UP, DOWN = 0, 1
STEPS = ((4, 3), (3, 4))


def kernel(
    wave_ref, proj_ref, table_ref, index_ref, count_ref, out_ref,
    bands, away, proj, table, index, acting, coefs, part, parts, weighted, result, sent, came, final, mix,
    ring_send, ring_recv, y_send, y_recv, c_send, c_recv, piece_send, piece_recv, pass_send, pass_recv,
    part_send, part_recv, wt_send, wt_recv, sum_send, sum_recv, end_send, end_recv, local_sem,
):
    rows, half = away.shape
    count = proj.shape[1]
    per_atom, _, kinds = table.shape
    share = rows // 2
    atom, band = lax.axis_index("atom"), lax.axis_index("band")
    y_lo, z, core = atom // (2 * Z), (atom // 2) % Z, atom % 2
    y_hi, x = band // SIDE, band % SIDE
    y = y_hi * 2 + y_lo
    me = y * SIDE + x
    slot = y_lo * 2 + core

    def at(lo, zz, cc, hi=y_hi, xx=x):
        return (lo * (2 * Z) + zz * 2 + cc, hi * SIDE + xx)

    mate = at(y_lo, z, 1 - core)
    across = at(1 - y_lo, z, core)
    corner = at(1 - y_lo, z, 1 - core)
    z_next = (at(y_lo, (z + 1) % Z, core), at(y_lo, (z + Z - 1) % Z, core))
    shifts = [(dy, dx) for dy in range(SIDE) for dx in range(SIDE) if dy or dx]

    def plane(dy, dx):
        yy, xx = (y + dy) % SIDE, (x + dx) % SIDE
        return yy * SIDE + xx, at(yy % 2, z, core, yy // 2, xx)

    def remote(src, dst, send, recv, to):
        return pltpu.make_async_remote_copy(
            src_ref=src, dst_ref=dst, send_sem=send, recv_sem=recv, device_id=to, device_id_type=MESH
        )

    mine = pl.ds(pl.multiple_of(y_lo * half, half), half)
    theirs = pl.ds(pl.multiple_of((1 - y_lo) * half, half), half)

    away_bands = pltpu.make_async_copy(wave_ref.at[:, theirs], away, local_sem.at[0])
    own_bands = pltpu.make_async_copy(wave_ref.at[:, mine], bands.at[y_lo, z], local_sem.at[1])
    own_proj = pltpu.make_async_copy(proj_ref.at[:, mine], proj.at[slot], local_sem.at[2])
    small = [
        pltpu.make_async_copy(table_ref, table, local_sem.at[3]),
        pltpu.make_async_copy(index_ref, index, local_sem.at[4]),
        pltpu.make_async_copy(count_ref, acting, local_sem.at[5]),
    ]
    for copy in (away_bands, own_bands, own_proj, *small):
        copy.start()

    barrier = pltpu.get_barrier_semaphore()
    greet = [mate, corner, *z_next] + [plane(*s)[1] for s in shifts]
    for to in greet:
        pl.semaphore_signal(barrier, inc=1, device_id=to, device_id_type=MESH)
    with scope("barrier"):
        pl.semaphore_wait(barrier, len(greet))

    started = []

    def go(copy):
        copy.start()
        started.append(copy)
        return copy

    def ring_copy(k, d, t):
        source = (z + Z - t) % Z if d == UP else (z + t) % Z
        block = bands.at[y_lo if k == 0 else 1 - y_lo, source]
        return remote(block, block, ring_send.at[k, d, t], ring_recv.at[k, d, t], z_next[d])

    away_bands.wait()
    y_bands = go(remote(away, bands.at[y_lo, z], y_send.at[0], y_recv.at[0], across))
    own_bands.wait()
    for d in (UP, DOWN):
        go(ring_copy(0, d, 0))
    size = count // PIECES
    pieces = [
        go(
            remote(
                proj_ref.at[pl.ds(i * size, size), theirs],
                proj.at[slot, pl.ds(i * size, size), :],
                piece_send.at[i], piece_recv.at[i], across,
            )
        )
        for i in range(PIECES)
    ]
    own_proj.wait()
    to_mate = go(remote(proj.at[slot], proj.at[slot], y_send.at[1], y_recv.at[1], mate))

    for copy in small:
        copy.wait()
    wide = (per_atom, count)
    lane = lax.broadcasted_iota(jnp.int32, wide, 1)
    inner = lane % per_atom
    chosen = jnp.zeros(wide, jnp.int32)
    limit = jnp.zeros(wide, jnp.int32)
    for a in range(count // per_atom):
        chosen = jnp.where(lane // per_atom == a, index[a], chosen)
        limit = jnp.where(lane // per_atom == a, acting[a], limit)
    kind = lax.broadcasted_iota(jnp.int32, (kinds, count), 0)
    value = jnp.zeros(wide, F32)
    for i in range(per_atom):
        pick = jnp.where((kind == chosen[:1]) & (inner[:1] == i), 1.0, 0.0).astype(F32)
        value += jnp.dot(table[i], pick, precision=lax.Precision.HIGHEST, preferred_element_type=F32)
    on = (inner < limit) & (lax.broadcasted_iota(jnp.int32, wide, 0) < limit)
    coefs[slot] = jnp.where(on, value, 0.0)

    with scope("ybands"):
        y_bands.wait_recv()
    for d in (UP, DOWN):
        go(ring_copy(1, d, 0))
    coef_copies = [
        go(remote(coefs.at[slot], coefs.at[slot], c_send.at[i], c_recv.at[i], to))
        for i, to in enumerate((mate, across, corner))
    ]
    far = (1 - y_lo) * 2 + core
    passed = []
    for t in range(4):
        for k in (0, 1):
            for d in (UP, DOWN):
                if t < STEPS[k][d]:
                    with scope(f"ag{t}{k}{d}"):
                        ring_copy(k, d, t).wait_recv()
                    if t + 1 < STEPS[k][d]:
                        go(ring_copy(k, d, t + 1))
        with scope(f"piece{t}"):
            pieces[t].wait_recv()
        block = proj.at[far, pl.ds(t * size, size), :]
        passed.append(go(remote(block, block, pass_send.at[t], pass_recv.at[t], mate)))

    for copy in coef_copies:
        copy.wait_recv()
    square = (count, count)
    same = lax.broadcasted_iota(jnp.int32, square, 0) // per_atom == lax.broadcasted_iota(jnp.int32, square, 1) // per_atom
    for s in range(4):
        mix[s] = jnp.where(same, jnp.concatenate([coefs[s]] * (count // per_atom), axis=0), 0.0)
    with scope("passed"):
        to_mate.wait_recv()
        for copy in passed:
            copy.wait_recv()

    group = Z * rows
    part_copies = [[], []]
    for g in (0, 1):
        with scope(f"S{g}"):

            @pl.loop(0, 2)
            def _(n):
                value = lax.dot_general(
                    bands[g].reshape(group, half),
                    proj[pl.ds(n * 2, 2)].reshape(2 * count, half),
                    (((1,), (1,)), ((), ())),
                    preferred_element_type=F32,
                )
                columns = pl.ds(pl.multiple_of(n * 2 * count, 2 * count), 2 * count)
                part[g, :, :, columns] = value.reshape(PLANE, share, 2 * count)

        for i, s in enumerate(shifts):
            chunk, to = plane(*s)
            part_copies[g].append(
                go(remote(part.at[g, chunk], parts.at[g, i], part_send.at[g, i], part_recv.at[g, i], to))
            )
    wt_copies = [[], []]
    for g in (0, 1):
        with scope(f"part{g}"):
            for copy in part_copies[g]:
                copy.wait_recv()
        with scope(f"mix{g}"):
            total = part[g, me]
            for i in range(len(shifts)):
                total += parts[g, i]
            mixed = [
                jnp.dot(
                    total[:, s * count : (s + 1) * count], mix[s],
                    precision=lax.Precision.HIGHEST, preferred_element_type=F32,
                )
                for s in range(4)
            ]
            weighted[g, me] = jnp.concatenate(mixed, axis=1).astype(BF16)
        for i, s in enumerate(shifts):
            _, to = plane(*s)
            block = weighted.at[g, me]
            wt_copies[g].append(go(remote(block, block, wt_send.at[g, i], wt_recv.at[g, i], to)))

    tile = 512
    width = half // 2

    def own_sum(g, h, owner):
        return result[g, owner, :, h * width : (h + 1) * width]

    def sum_copy(g, h, d, t):
        return remote(
            sent.at[g, h, d, t], came.at[g, h, d, t], sum_send.at[g, h, d, t], sum_recv.at[g, h, d, t], z_next[d]
        )

    def sum_step(g, h, d, t):
        n = STEPS[h][d]
        owner = (z + (n - t)) % Z if d == UP else (z + Z - (n - t)) % Z
        value = own_sum(g, h, owner)
        if t > 0:
            with scope(f"rs{t - 1}{g}{h}{d}"):
                sum_copy(g, h, d, t - 1).wait_recv()
            value += came[g, h, d, t - 1].astype(F32)
        sent[g, h, d, t] = value.astype(BF16)
        go(sum_copy(g, h, d, t))

    for g in (0, 1):
        with scope(f"wt{g}"):
            for copy in wt_copies[g]:
                copy.wait_recv()
        for h in (0, 1):
            with scope(f"O{g}{h}"):

                @pl.loop(0, width // tile)
                def _(n):
                    columns = pl.ds(pl.multiple_of(h * width + n * tile, tile), tile)
                    value = jnp.dot(
                        weighted[g].reshape(group, 4 * count),
                        proj[:, :, columns].reshape(4 * count, tile),
                        preferred_element_type=F32,
                    )
                    result[g, :, :, columns] = value.reshape(Z, rows, tile)

            for d in (UP, DOWN):
                sum_step(g, h, d, 0)
    for t in range(1, 4):
        for g in (0, 1):
            for h in (0, 1):
                for d in (UP, DOWN):
                    if t < STEPS[h][d]:
                        sum_step(g, h, d, t)
    ends = []
    for g in (0, 1):
        for h in (0, 1):
            value = own_sum(g, h, z)
            for d in (UP, DOWN):
                last = STEPS[h][d] - 1
                with scope(f"rs{last}{g}{h}{d}"):
                    sum_copy(g, h, d, last).wait_recv()
                value += came[g, h, d, last].astype(F32)
            final[g, :, h * width : (h + 1) * width] = value.astype(BF16)
            columns = pl.ds(pl.multiple_of(y_lo * half + h * width, width), width)
            there = remote(
                final.at[g, :, pl.ds(h * width, width)], out_ref.at[:, columns], end_send.at[h], end_recv.at[h], across
            )
            here = pltpu.make_async_copy(
                final.at[g, :, pl.ds(h * width, width)], out_ref.at[:, columns], local_sem.at[6 + h]
            )

            @pl.when(y_lo == g)
            def _():
                here.start()

            @pl.when(y_lo != g)
            def _():
                there.start()

            if g == 0:
                ends.append((there, here))
    with scope("ends"):
        for there, here in ends:
            there.wait_recv()
            here.wait()
    with scope("drain"):
        for there, _ in ends:
            there.wait_send()
        for copy in started:
            copy.wait_send()


def shards(wave_rows, projectors, dij_table, dij_index, proj_count):
    rows, width = wave_rows.shape
    count = projectors.shape[0]
    half = width // 2
    kinds, per_atom, _ = dij_table.shape
    atoms = count // per_atom

    dma = pltpu.SemaphoreType.DMA
    others = PLANE - 1
    hbm = pl.BlockSpec(memory_space=pltpu.MemorySpace.HBM)
    return pl.pallas_call(
        kernel,
        out_shape=jax.ShapeDtypeStruct((rows, width), BF16),
        in_specs=[hbm] * 5,
        out_specs=pl.BlockSpec(memory_space=pl.ANY),
        scratch_shapes=[
            pltpu.VMEM((2, Z, rows, half), BF16),
            pltpu.VMEM((rows, half), BF16),
            pltpu.VMEM((4, count, half), BF16),
            pltpu.VMEM((per_atom, per_atom, kinds), F32),
            pltpu.SMEM((atoms,), jnp.int32),
            pltpu.SMEM((atoms,), jnp.int32),
            pltpu.VMEM((4, per_atom, count), F32),
            pltpu.VMEM((2, PLANE, rows // 2, 4 * count), F32),
            pltpu.VMEM((2, others, rows // 2, 4 * count), F32),
            pltpu.VMEM((2, PLANE, rows // 2, 4 * count), BF16),
            pltpu.VMEM((2, Z, rows, half), F32),
            pltpu.VMEM((2, 2, 2, 4, rows, half // 2), BF16),
            pltpu.VMEM((2, 2, 2, 4, rows, half // 2), BF16),
            pltpu.VMEM((2, rows, half), BF16),
            pltpu.VMEM((4, count, count), F32),
            dma((2, 2, 4)), dma((2, 2, 4)),
            dma((2,)), dma((2,)),
            dma((3,)), dma((3,)),
            dma((PIECES,)), dma((PIECES,)),
            dma((PIECES,)), dma((PIECES,)),
            dma((2, others)), dma((2, others)),
            dma((2, others)), dma((2, others)),
            dma((2, 2, 2, 4)), dma((2, 2, 2, 4)),
            dma((2,)), dma((2,)),
            dma((8,)),
        ],
        compiler_params=pltpu.CompilerParams(
            collective_id=0, has_side_effects=True, vmem_limit_bytes=67_043_328
        ),
        name="nonlocal_rows",
    )(wave_rows, projectors, jnp.transpose(dij_table, (1, 2, 0)), dij_index, proj_count)


def solution(mesh):
    return jax.shard_map(
        shards,
        mesh=mesh,
        in_specs=(P("atom", "band"), P("atom", "band"), P(), P("atom"), P("atom")),
        out_specs=P("atom", "band"),
        check_vma=False,
    )
```

```python
import functools

import jax
import jax.numpy as jnp
from jax import lax
from jax.experimental import pallas as pl
from jax.experimental.pallas import tpu as pltpu
from jax.sharding import PartitionSpec as P

MESH = pl.DeviceIdType.MESH
F32 = jnp.float32
BF16 = jnp.bfloat16
scope = jax.named_scope
Z = 8
SIDE = 4
PLANE = SIDE * SIDE
WIDTHS = (1024, 1024, 896, 896, 256)
PARTS = len(WIDTHS)
ALONE = 256
PIECE = 1024
UP, DOWN = 0, 1
RING, ACROSS, PIECE_SEND, MATE, COEFS, PASS, PART, WEIGHTED, SUM, SWAP, END = range(11)
SENDS = 11
STEPS = ((4, 3), (3, 4), (4, 3), (3, 4), (3, 4))


def kernel(
    wave_ref, proj_ref, table_ref, index_ref, count_ref, out_ref,
    bands, away, proj, table, index, acting, coefs, part, parts, weighted, result, sent, came, swap_out, swap_in, final, mix,
    send_sem, ring_recv, y_recv, mate_recv, c_recv, piece_recv, pass_recv, part_recv, wt_recv, sum_recv, swap_recv, end_recv,
    local_sem,
):
    rows, wide = away.shape
    half = wide - ALONE
    both = half - ALONE
    count = proj.shape[2]
    per_atom, _, kinds = table.shape
    share = rows // 2
    atom, band = lax.axis_index("atom"), lax.axis_index("band")
    y_lo, z, core = atom // (2 * Z), (atom // 2) % Z, atom % 2
    y_hi, x = band // SIDE, band % SIDE
    y = y_hi * 2 + y_lo
    me = y * SIDE + x
    slot = y_lo * 2 + core

    def at(lo, zz, cc, hi=y_hi, xx=x):
        return (lo * (2 * Z) + zz * 2 + cc, hi * SIDE + xx)

    mate = at(y_lo, z, 1 - core)
    across = at(1 - y_lo, z, core)
    corner = at(1 - y_lo, z, 1 - core)
    z_next = (at(y_lo, (z + 1) % Z, core), at(y_lo, (z + Z - 1) % Z, core))
    shifts = [(dy, dx) for dy in range(SIDE) for dx in range(SIDE) if dy or dx]
    shifts.sort(key=lambda s: -min(s[0], SIDE - s[0]) - min(s[1], SIDE - s[1]))

    def plane(dy, dx):
        yy, xx = (y + dy) % SIDE, (x + dx) % SIDE
        return yy * SIDE + xx, at(yy % 2, z, core, yy // 2, xx)

    def remote(src, dst, send, recv, to):
        return pltpu.make_async_remote_copy(
            src_ref=src, dst_ref=dst, send_sem=send, recv_sem=recv, device_id=to, device_id_type=MESH
        )

    def columns_of(side, first, size):
        return pl.ds(pl.multiple_of(side * half + first, 128), size)

    mine, theirs = columns_of(y_lo, 0, half), columns_of(1 - y_lo, 0, half)
    mine_alone, theirs_alone = columns_of(y_lo, both, ALONE), columns_of(1 - y_lo, both, ALONE)
    body, rest = pl.ds(0, half), pl.ds(half, ALONE)

    away_bands = [
        pltpu.make_async_copy(wave_ref.at[:, theirs], away.at[:, body], local_sem.at[0]),
        pltpu.make_async_copy(wave_ref.at[:, mine_alone], away.at[:, rest], local_sem.at[1]),
    ]
    own_bands = [
        pltpu.make_async_copy(wave_ref.at[:, mine], bands.at[y_lo, z, :, body], local_sem.at[2]),
        pltpu.make_async_copy(wave_ref.at[:, theirs_alone], bands.at[y_lo, z, :, rest], local_sem.at[3]),
    ]
    own_proj = [
        pltpu.make_async_copy(proj_ref.at[:, mine], proj.at[y_lo, core, :, body], local_sem.at[4]),
        pltpu.make_async_copy(proj_ref.at[:, theirs_alone], proj.at[y_lo, core, :, rest], local_sem.at[5]),
    ]
    small = [
        pltpu.make_async_copy(table_ref, table, local_sem.at[6]),
        pltpu.make_async_copy(index_ref, index, local_sem.at[7]),
        pltpu.make_async_copy(count_ref, acting, local_sem.at[8]),
    ]
    for copy in (*away_bands, *own_bands, *own_proj, *small):
        copy.start()

    barrier = pltpu.get_barrier_semaphore()
    greet = [mate, corner, *z_next] + [plane(*s)[1] for s in shifts]
    for to in greet:
        pl.semaphore_signal(barrier, inc=1, device_id=to, device_id_type=MESH)
    with scope("barrier"):
        pl.semaphore_wait(barrier, len(greet))

    def go(copy):
        copy.start()
        return copy

    def sent_all(ref, sem):
        remote(ref, ref, sem, sem, mate).wait_send()

    def got_all(ref, sem):
        remote(ref, ref, sem, sem, mate).wait_recv()

    def ring_copy(k, h, d, t):
        source = (z + Z - t) % Z if d == UP else (z + t) % Z
        block = bands.at[y_lo if k == 0 else 1 - y_lo, source, :, pl.ds(h * (wide // 2), wide // 2)]
        return remote(block, block, send_sem.at[RING], ring_recv.at[k, h, d * STEPS[h][UP] + t], z_next[d])

    for copy in away_bands:
        copy.wait()
    y_bands = []
    for h in (0, 1):
        columns = pl.ds(h * (wide // 2), wide // 2)
        y_bands.append(
            go(remote(away.at[:, columns], bands.at[y_lo, z, :, columns], send_sem.at[ACROSS], y_recv.at[h], across))
        )
    for copy in own_bands:
        copy.wait()
    for h in (0, 1):
        for d in (UP, DOWN):
            go(ring_copy(0, h, d, 0))
    cuts = [(first, min(PIECE, both - first)) for first in range(0, both, PIECE)]
    pieces = [
        remote(
            proj_ref.at[:, columns_of(1 - y_lo, first, size)], proj.at[y_lo, core, :, pl.ds(first, size)],
            send_sem.at[PIECE_SEND], piece_recv.at[i], across,
        )
        for i, (first, size) in enumerate(cuts)
    ]
    for copy in pieces[:2]:
        go(copy)
    for copy in own_proj:
        copy.wait()
    there = proj.at[y_lo, core]
    to_mate = go(remote(there, there, send_sem.at[MATE], mate_recv.at[0], mate))

    for copy in small:
        copy.wait()
    flat = (per_atom, count)
    lane = lax.broadcasted_iota(jnp.int32, flat, 1)
    inner = lane % per_atom
    chosen = jnp.zeros(flat, jnp.int32)
    limit = jnp.zeros(flat, jnp.int32)
    for a in range(count // per_atom):
        chosen = jnp.where(lane // per_atom == a, index[a], chosen)
        limit = jnp.where(lane // per_atom == a, acting[a], limit)
    kind = lax.broadcasted_iota(jnp.int32, (kinds, count), 0)
    value = jnp.zeros(flat, F32)
    for i in range(per_atom):
        pick = jnp.where((kind == chosen[:1]) & (inner[:1] == i), 1.0, 0.0).astype(F32)
        value += jnp.dot(table[i], pick, precision=lax.Precision.HIGHEST, preferred_element_type=F32)
    on = (inner < limit) & (lax.broadcasted_iota(jnp.int32, flat, 0) < limit)
    coefs[slot] = jnp.where(on, value, 0.0)

    coef_copies = [
        go(remote(coefs.at[slot], coefs.at[slot], send_sem.at[COEFS], c_recv.at[i], to))
        for i, to in enumerate((mate, across, corner))
    ]
    for copy in pieces[2:]:
        go(copy)
    for h in (0, 1):
        with scope(f"ybands{h}"):
            y_bands[h].wait_recv()
        for d in (UP, DOWN):
            go(ring_copy(1, h, d, 0))
    passed = []

    def pass_piece(i):
        with scope(f"piece{i}"):
            pieces[i].wait_recv()
        first, size = cuts[i]
        there = proj.at[1 - y_lo, core, :, pl.ds(first, size)]
        passed.append(go(remote(there, there, send_sem.at[PASS], pass_recv.at[i], mate)))

    def contract(lines, kept):
        return lax.dot_general(lines, kept, (((1,), (1,)), ((), ())), preferred_element_type=F32)

    own_pair = pl.ds(pl.multiple_of(y_lo * 2 * count, count), 2 * count)
    far_pair = pl.ds(pl.multiple_of((1 - y_lo) * 2 * count, count), 2 * count)

    def own_parts(sources):
        lines = [bands[:, source].reshape(2 * rows, wide) for source in sources]
        kept = proj[y_lo].reshape(2 * count, wide)
        value = contract(kept, lines[0]).T if len(lines) == 1 else contract(jnp.concatenate(lines, axis=0), kept)
        for i, source in enumerate(sources):
            here = value[i * 2 * rows : (i + 1) * 2 * rows].reshape(2, 2, share, 2 * count)
            part[:, pl.ds(source * 2, 2), :, own_pair] = here

    def send_parts(g, columns):
        for i, s in enumerate(shifts):
            chunk, to = plane(*s)
            go(
                remote(
                    part.at[g, chunk, :, columns], parts.at[g, i, :, columns], send_sem.at[PART], part_recv.at[g], to
                )
            )

    for t in range(4):
        for k in (0, 1):
            for h in (0, 1):
                for d in (UP, DOWN):
                    if t < STEPS[h][d]:
                        with scope(f"ag{t}{k}{h}{d}"):
                            ring_copy(k, h, d, t).wait_recv()
                        if t + 1 < STEPS[h][d]:
                            go(ring_copy(k, h, d, t + 1))
        if t < 3:
            pass_piece(t)
        if t == 0:
            with scope("tomate"):
                to_mate.wait_recv()
            with scope("S00"):
                own_parts([z])
        with scope(f"S{t + 1}"):
            up, down = (z + Z - t - 1) % Z, (z + t + 1) % Z
            own_parts([up, down] if t < 3 else [up])
    send_parts(0, own_pair)
    pass_piece(3)

    every = 2 * Z * rows
    ready = cuts[3][0]
    with scope("passed0"):
        for copy in passed[:3]:
            copy.wait_recv()
    with scope("Sfar0"):
        value = contract(
            bands[:, :, :, :ready].reshape(every, ready), proj[1 - y_lo, :, :, :ready].reshape(2 * count, ready)
        )
        part[:, :, :, far_pair] = value.reshape(2, PLANE, share, 2 * count)
    with scope("mixes"):
        for copy in coef_copies:
            copy.wait_recv()
        square = (count, count)
        down = lax.broadcasted_iota(jnp.int32, square, 0)
        same = down // per_atom == lax.broadcasted_iota(jnp.int32, square, 1) // per_atom
        for s in range(4):
            mix[s] = jnp.where(same, jnp.concatenate([coefs[s]] * (count // per_atom), axis=0), 0.0)
    with scope("passed"):
        passed[3].wait_recv()
    with scope("Sfar1"):
        value = contract(
            bands[:, :, :, ready:both].reshape(every, both - ready),
            proj[1 - y_lo, :, :, ready:both].reshape(2 * count, both - ready),
        )
        part[:, :, :, far_pair] += value.reshape(2, PLANE, share, 2 * count)
    send_parts(0, far_pair)
    send_parts(1, own_pair)
    send_parts(1, far_pair)
    for g in (0, 1):
        with scope(f"part{g}"):
            got_all(parts.at[g], part_recv.at[g])
        with scope(f"mix{g}"):
            total = part[g, me]
            for i in range(len(shifts)):
                total += parts[g, i]
            mixed = [
                jnp.dot(
                    total[:, s * count : (s + 1) * count], mix[s],
                    precision=lax.Precision.HIGHEST, preferred_element_type=F32,
                )
                for s in range(4)
            ]
            weighted[g, me] = jnp.concatenate(mixed, axis=1).astype(BF16)
        for i, s in enumerate(shifts):
            _, to = plane(*s)
            there = weighted.at[g, me]
            go(remote(there, there, send_sem.at[WEIGHTED], wt_recv.at[g], to))

    group = Z * rows
    tile = 512
    starts = [sum(WIDTHS[:h]) for h in range(PARTS)]
    spans = [slice(first, first + size) for first, size in zip(starts, WIDTHS)]

    def own_sum(g, h, owner):
        return result[g, owner, :, spans[h]]

    def at_step(h, d, t):
        return d * STEPS[h][UP] + t

    def sum_copy(g, h, d, t):
        n = at_step(h, d, t)
        size = pl.ds(0, WIDTHS[h])
        return remote(
            sent.at[g, h, n, :, size], came.at[g, h, n, :, size], send_sem.at[SUM], sum_recv.at[g, h, n], z_next[d]
        )

    def arrived(g, h, d, t):
        return came[g, h, at_step(h, d, t), :, : WIDTHS[h]].astype(F32)

    def sum_step(g, h, d, t):
        n = STEPS[h][d]
        owner = (z + (n - t)) % Z if d == UP else (z + Z - (n - t)) % Z
        value = own_sum(g, h, owner)
        if t > 0:
            with scope(f"rs{t - 1}{h}{d}"):
                sum_copy(g, h, d, t - 1).wait_recv()
            value += arrived(g, h, d, t - 1)
        sent[g, h, at_step(h, d, t), :, : WIDTHS[h]] = value.astype(BF16)
        go(sum_copy(g, h, d, t))

    swaps = []
    for g in (0, 1):
        with scope(f"wt{g}"):
            got_all(weighted.at[g, pl.ds(0, PLANE - 1)], wt_recv.at[g])
        with scope(f"alone{g}"):
            value = jnp.dot(
                weighted[g, :, :, own_pair].reshape(group, 2 * count),
                proj[y_lo, :, :, both:].reshape(2 * count, 2 * ALONE),
                preferred_element_type=F32,
            ).reshape(Z, rows, 2 * ALONE)
            result[g, :, :, both:] = value[:, :, :ALONE]
            swap_out[g] = value[:, :, ALONE:].astype(BF16)
            swaps.append(go(remote(swap_out.at[g], swap_in.at[g], send_sem.at[SWAP], swap_recv.at[g], across)))
        for h in range(PARTS - 1):
            with scope(f"O{g}{h}"):
                for first in range(spans[h].start, spans[h].stop, tile):
                    size = min(tile, spans[h].stop - first)
                    value = jnp.dot(
                        weighted[g].reshape(group, 4 * count),
                        proj[:, :, :, first : first + size].reshape(4 * count, size),
                        preferred_element_type=F32,
                    )
                    result[g, :, :, first : first + size] = value.reshape(Z, rows, size)
            for d in (UP, DOWN):
                sum_step(g, h, d, 0)
    tail = PARTS - 1
    order = [(g, h, t) for g in (0, 1) for h, t in [(tail, 0)] + [(h, 1) for h in range(tail)]]
    order += [(g, tail, 1) for g in (0, 1)] + [(g, h, 2) for h in range(tail) for g in (0, 1)]
    order += [(g, tail, 2) for g in (0, 1)] + [(g, h, 3) for g in (1 - y_lo, y_lo) for h in (tail, *range(tail))]
    for g, h, t in order:
        if t == 0:
            with scope(f"swap{g}"):
                swaps[g].wait_recv()
            result[g, :, :, both:] = result[g, :, :, both:] + swap_in[g].astype(F32)
        for d in (UP, DOWN):
            if t < STEPS[h][d]:
                sum_step(g, h, d, t)
    ends = []
    for far_rows, g in ((True, 1 - y_lo), (False, y_lo)):
        for h in (tail, *range(tail)):
            value = own_sum(g, h, z)
            for d in (UP, DOWN):
                last = STEPS[h][d] - 1
                with scope(f"rs{last}{h}{d}{far_rows}"):
                    sum_copy(g, h, d, last).wait_recv()
                value += arrived(g, h, d, last)
            there = final.at[g, :, spans[h]]
            final[g, :, spans[h]] = value.astype(BF16)
            columns = columns_of(y_lo, starts[h], WIDTHS[h])
            if far_rows:
                go(remote(there, out_ref.at[:, columns], send_sem.at[END], end_recv.at[0], across))
            else:
                ends.append(pltpu.make_async_copy(there, out_ref.at[:, columns], local_sem.at[h]))
                ends[-1].start()
    with scope("ends"):
        got_all(final.at[0], end_recv.at[0])
        for copy in ends:
            copy.wait()
    with scope("drain"):
        sent_all(final.at[0], send_sem.at[END])
        sent_all(bands.at[:, pl.ds(0, Z - 1)], send_sem.at[RING])
        sent_all(away, send_sem.at[ACROSS])
        sent_all(proj.at[0, 0, :, pl.ds(0, both)], send_sem.at[PIECE_SEND])
        sent_all(proj.at[0, 0], send_sem.at[MATE])
        sent_all(coefs.at[pl.ds(0, 3)], send_sem.at[COEFS])
        sent_all(proj.at[0, 0, :, pl.ds(0, both)], send_sem.at[PASS])
        sent_all(parts, send_sem.at[PART])
        sent_all(weighted.at[:, pl.ds(0, PLANE - 1)], send_sem.at[WEIGHTED])
        sent_all(swap_out, send_sem.at[SWAP])
        sent_all(bands.at[:, pl.ds(0, Z - 1), :, pl.ds(0, half)], send_sem.at[SUM])


def shards(wave_rows, projectors, dij_table, dij_index, proj_count):
    rows, width = wave_rows.shape
    count = projectors.shape[0]
    half = width // 2
    wide = half + ALONE
    kinds, per_atom, _ = dij_table.shape
    atoms = count // per_atom

    dma = pltpu.SemaphoreType.DMA
    others = PLANE - 1
    hbm = pl.BlockSpec(memory_space=pltpu.MemorySpace.HBM)
    return pl.pallas_call(
        kernel,
        out_shape=jax.ShapeDtypeStruct((rows, width), BF16),
        in_specs=[hbm] * 5,
        out_specs=pl.BlockSpec(memory_space=pl.ANY),
        scratch_shapes=[
            pltpu.VMEM((2, Z, rows, wide), BF16),
            pltpu.VMEM((rows, wide), BF16),
            pltpu.VMEM((2, 2, count, wide), BF16),
            pltpu.VMEM((per_atom, per_atom, kinds), F32),
            pltpu.SMEM((atoms,), jnp.int32),
            pltpu.SMEM((atoms,), jnp.int32),
            pltpu.VMEM((4, per_atom, count), F32),
            pltpu.VMEM((2, PLANE, rows // 2, 4 * count), F32),
            pltpu.VMEM((2, others, rows // 2, 4 * count), F32),
            pltpu.VMEM((2, PLANE, rows // 2, 4 * count), BF16),
            pltpu.VMEM((2, Z, rows, half), F32),
            pltpu.VMEM((2, PARTS, Z - 1, rows, max(WIDTHS)), BF16),
            pltpu.VMEM((2, PARTS, Z - 1, rows, max(WIDTHS)), BF16),
            pltpu.VMEM((2, Z, rows, ALONE), BF16),
            pltpu.VMEM((2, Z, rows, ALONE), BF16),
            pltpu.VMEM((2, rows, half), BF16),
            pltpu.VMEM((4, count, count), F32),
            dma((SENDS,)),
            dma((2, 2, Z - 1)),
            dma((2,)),
            dma((1,)),
            dma((3,)),
            dma((4,)),
            dma((4,)),
            dma((2,)),
            dma((2,)),
            dma((2, PARTS, Z - 1)),
            dma((2,)),
            dma((1,)),
            dma((9,)),
        ],
        compiler_params=pltpu.CompilerParams(
            collective_id=0, has_side_effects=True, vmem_limit_bytes=67_043_328
        ),
        name="nonlocal_rows",
    )(wave_rows, projectors, jnp.transpose(dij_table, (1, 2, 0)), dij_index, proj_count)


def solution(mesh):
    return jax.shard_map(
        shards,
        mesh=mesh,
        in_specs=(P("atom", "band"), P("atom", "band"), P(), P("atom"), P("atom")),
        out_specs=P("atom", "band"),
        check_vma=False,
    )
```

```python
import functools

import jax
import jax.numpy as jnp
from jax import lax
from jax.experimental import pallas as pl
from jax.experimental.pallas import tpu as pltpu
from jax.sharding import PartitionSpec as P

MESH = pl.DeviceIdType.MESH
F32 = jnp.float32
BF16 = jnp.bfloat16
scope = jax.named_scope
Z = 8
SIDE = 4
PLANE = SIDE * SIDE
PARTS = 4
PIECES = (1024, 1024, 1024, 768, 256)
UP, DOWN = 0, 1
RING, ACROSS, PIECE_SEND, MATE, COEFS, PASS, PART, WEIGHTED, SUM, END = range(10)
SENDS = 10
STEPS = ((4, 3), (3, 4), (4, 3), (3, 4))


def kernel(
    wave_ref, proj_ref, table_ref, index_ref, count_ref, out_ref,
    bands, away, proj, table, index, acting, coefs, part, parts, weighted, result, sent, came, last, across_share, final, mix,
    send_sem, ring_recv, y_recv, mate_recv, c_recv, piece_recv, pass_recv, part_recv, wt_recv, sum_recv, last_recv, end_recv,
    local_sem,
):
    rows, half = away.shape
    count = proj.shape[2]
    per_atom, _, kinds = table.shape
    share = rows // 2
    atom, band = lax.axis_index("atom"), lax.axis_index("band")
    y_lo, z, core = atom // (2 * Z), (atom // 2) % Z, atom % 2
    y_hi, x = band // SIDE, band % SIDE
    y = y_hi * 2 + y_lo
    me = y * SIDE + x
    slot = y_lo * 2 + core

    def at(lo, zz, cc, hi=y_hi, xx=x):
        return (lo * (2 * Z) + zz * 2 + cc, hi * SIDE + xx)

    mate = at(y_lo, z, 1 - core)
    across = at(1 - y_lo, z, core)
    corner = at(1 - y_lo, z, 1 - core)
    z_next = (at(y_lo, (z + 1) % Z, core), at(y_lo, (z + Z - 1) % Z, core))
    shifts = [(dy, dx) for dy in range(SIDE) for dx in range(SIDE) if dy or dx]
    shifts.sort(key=lambda s: -min(s[0], SIDE - s[0]) - min(s[1], SIDE - s[1]))

    def plane(dy, dx):
        yy, xx = (y + dy) % SIDE, (x + dx) % SIDE
        return yy * SIDE + xx, at(yy % 2, z, core, yy // 2, xx)

    def remote(src, dst, send, recv, to):
        return pltpu.make_async_remote_copy(
            src_ref=src, dst_ref=dst, send_sem=send, recv_sem=recv, device_id=to, device_id_type=MESH
        )

    def columns_of(side, first, size):
        return pl.ds(pl.multiple_of(side * half + first, 128), size)

    mine, theirs = columns_of(y_lo, 0, half), columns_of(1 - y_lo, 0, half)
    away_bands = pltpu.make_async_copy(wave_ref.at[:, theirs], away, local_sem.at[0])
    own_bands = pltpu.make_async_copy(wave_ref.at[:, mine], bands.at[y_lo, z], local_sem.at[1])
    own_proj = pltpu.make_async_copy(proj_ref.at[:, mine], proj.at[y_lo, core], local_sem.at[2])
    small = [
        pltpu.make_async_copy(table_ref, table, local_sem.at[3]),
        pltpu.make_async_copy(index_ref, index, local_sem.at[4]),
        pltpu.make_async_copy(count_ref, acting, local_sem.at[5]),
    ]
    for copy in (away_bands, own_bands, own_proj, *small):
        copy.start()

    barrier = pltpu.get_barrier_semaphore()
    slant = (at(1 - y_lo, (z + 1) % Z, core), at(1 - y_lo, (z + Z - 1) % Z, core))
    greet = [mate, corner, *z_next, *slant] + [plane(*s)[1] for s in shifts]
    for to in greet:
        pl.semaphore_signal(barrier, inc=1, device_id=to, device_id_type=MESH)
    with scope("barrier"):
        pl.semaphore_wait(barrier, len(greet))

    def go(copy):
        copy.start()
        return copy

    def sent_all(ref, sem):
        remote(ref, ref, sem, sem, mate).wait_send()

    def got_all(ref, sem):
        remote(ref, ref, sem, sem, mate).wait_recv()

    def ring_copy(k, h, d, t):
        source = (z + Z - t) % Z if d == UP else (z + t) % Z
        block = bands.at[y_lo if k == 0 else 1 - y_lo, source, :, pl.ds(h * (half // 2), half // 2)]
        return remote(block, block, send_sem.at[RING], ring_recv.at[k, h, d * STEPS[h][UP] + t], z_next[d])

    away_bands.wait()
    y_bands = []
    for h in (0, 1):
        columns = pl.ds(h * (half // 2), half // 2)
        y_bands.append(
            go(remote(away.at[:, columns], bands.at[y_lo, z, :, columns], send_sem.at[ACROSS], y_recv.at[h], across))
        )
    own_bands.wait()
    for h in (0, 1):
        for d in (UP, DOWN):
            go(ring_copy(0, h, d, 0))
    cuts = [(sum(PIECES[:i]), size) for i, size in enumerate(PIECES)]
    pieces = [
        remote(
            proj_ref.at[:, columns_of(1 - y_lo, first, size)], proj.at[y_lo, core, :, pl.ds(first, size)],
            send_sem.at[PIECE_SEND], piece_recv.at[i], across,
        )
        for i, (first, size) in enumerate(cuts)
    ]
    for copy in pieces[:2]:
        go(copy)
    own_proj.wait()
    there = proj.at[y_lo, core]
    to_mate = go(remote(there, there, send_sem.at[MATE], mate_recv.at[0], mate))

    for copy in small:
        copy.wait()
    flat = (per_atom, count)
    lane = lax.broadcasted_iota(jnp.int32, flat, 1)
    inner = lane % per_atom
    chosen = jnp.zeros(flat, jnp.int32)
    limit = jnp.zeros(flat, jnp.int32)
    for a in range(count // per_atom):
        chosen = jnp.where(lane // per_atom == a, index[a], chosen)
        limit = jnp.where(lane // per_atom == a, acting[a], limit)
    kind = lax.broadcasted_iota(jnp.int32, (kinds, count), 0)
    value = jnp.zeros(flat, F32)
    for i in range(per_atom):
        pick = jnp.where((kind == chosen[:1]) & (inner[:1] == i), 1.0, 0.0).astype(F32)
        value += jnp.dot(table[i], pick, precision=lax.Precision.HIGHEST, preferred_element_type=F32)
    on = (inner < limit) & (lax.broadcasted_iota(jnp.int32, flat, 0) < limit)
    coefs[slot] = jnp.where(on, value, 0.0)

    coef_copies = [
        go(remote(coefs.at[slot], coefs.at[slot], send_sem.at[COEFS], c_recv.at[i], to))
        for i, to in enumerate((mate, across, corner))
    ]
    for copy in pieces[2:]:
        go(copy)
    for h in (0, 1):
        with scope(f"ybands{h}"):
            y_bands[h].wait_recv()
        for d in (UP, DOWN):
            go(ring_copy(1, h, d, 0))
    passed = []

    def pass_piece(i):
        with scope(f"piece{i}"):
            pieces[i].wait_recv()
        first, size = cuts[i]
        there = proj.at[1 - y_lo, core, :, pl.ds(first, size)]
        passed.append(go(remote(there, there, send_sem.at[PASS], pass_recv.at[i], mate)))

    def contract(lines, kept):
        return lax.dot_general(lines, kept, (((1,), (1,)), ((), ())), preferred_element_type=F32)

    own_pair = pl.ds(pl.multiple_of(y_lo * 2 * count, count), 2 * count)
    far_pair = pl.ds(pl.multiple_of((1 - y_lo) * 2 * count, count), 2 * count)

    def own_parts(sources):
        lines = [bands[:, source].reshape(2 * rows, half) for source in sources]
        kept = proj[y_lo].reshape(2 * count, half)
        value = contract(kept, lines[0]).T if len(lines) == 1 else contract(jnp.concatenate(lines, axis=0), kept)
        for i, source in enumerate(sources):
            here = value[i * 2 * rows : (i + 1) * 2 * rows].reshape(2, 2, share, 2 * count)
            part[:, pl.ds(source * 2, 2), :, own_pair] = here

    def send_parts(g, columns):
        for i, s in enumerate(shifts):
            chunk, to = plane(*s)
            go(
                remote(
                    part.at[g, chunk, :, columns], parts.at[g, i, :, columns], send_sem.at[PART], part_recv.at[g], to
                )
            )

    for t in range(4):
        for k in (0, 1):
            for h in (0, 1):
                for d in (UP, DOWN):
                    if t < STEPS[h][d]:
                        with scope(f"ag{t}{k}{h}{d}"):
                            ring_copy(k, h, d, t).wait_recv()
                        if t + 1 < STEPS[h][d]:
                            go(ring_copy(k, h, d, t + 1))
        if t == 1:
            pass_piece(0)
            with scope("tomate"):
                to_mate.wait_recv()
            with scope("S1"):
                own_parts([(z + Z + i) % Z for i in range(-2, 3)])
        if t == 2:
            pass_piece(1)
            with scope("S2"):
                own_parts([(z + Z - 3) % Z, (z + 3) % Z])
            pass_piece(2)
    with scope("S3"):
        own_parts([(z + 4) % Z])
    send_parts(0, own_pair)

    every = 2 * Z * rows
    ready = cuts[3][0]
    with scope("passed0"):
        for copy in passed:
            copy.wait_recv()
    with scope("Sfar0"):
        value = contract(
            bands[:, :, :, :ready].reshape(every, ready), proj[1 - y_lo, :, :, :ready].reshape(2 * count, ready)
        )
        part[:, :, :, far_pair] = value.reshape(2, PLANE, share, 2 * count)
    pass_piece(3)
    pass_piece(4)
    with scope("mixes"):
        for copy in coef_copies:
            copy.wait_recv()
        square = (count, count)
        down = lax.broadcasted_iota(jnp.int32, square, 0)
        same = down // per_atom == lax.broadcasted_iota(jnp.int32, square, 1) // per_atom
        for s in range(4):
            mix[s] = jnp.where(same, jnp.concatenate([coefs[s]] * (count // per_atom), axis=0), 0.0)
    with scope("passed"):
        for copy in passed[3:]:
            copy.wait_recv()
    with scope("Sfar1"):
        value = contract(
            bands[:, :, :, ready:].reshape(every, half - ready),
            proj[1 - y_lo, :, :, ready:].reshape(2 * count, half - ready),
        )
        part[:, :, :, far_pair] += value.reshape(2, PLANE, share, 2 * count)
    send_parts(0, far_pair)
    send_parts(1, own_pair)
    send_parts(1, far_pair)
    for g in (0, 1):
        with scope(f"part{g}"):
            got_all(parts.at[g], part_recv.at[g])
        with scope(f"mix{g}"):
            total = part[g, me]
            for i in range(len(shifts)):
                total += parts[g, i]
            mixed = [
                jnp.dot(
                    total[:, s * count : (s + 1) * count], mix[s],
                    precision=lax.Precision.HIGHEST, preferred_element_type=F32,
                )
                for s in range(4)
            ]
            weighted[g, me] = jnp.concatenate(mixed, axis=1).astype(BF16)
        for i, s in enumerate(shifts):
            _, to = plane(*s)
            there = weighted.at[g, me]
            go(remote(there, there, send_sem.at[WEIGHTED], wt_recv.at[g], to))

    group = Z * rows
    tile = 512
    width = half // PARTS
    spans = [slice(h * width, (h + 1) * width) for h in range(PARTS)]

    def own_sum(g, h, owner):
        return result[g, owner, :, spans[h]]

    def at_step(h, d, t):
        return d * STEPS[h][UP] + t

    def sum_copy(g, h, d, t):
        n = at_step(h, d, t)
        if t < STEPS[h][d] - 1:
            return remote(
                sent.at[g, h, n], came.at[g, h, n], send_sem.at[SUM], sum_recv.at[g, h, n - d], z_next[d]
            )
        owner = at(g, (z + 1) % Z if d == UP else (z + Z - 1) % Z, core)
        return remote(sent.at[g, h, n], last.at[y_lo, h, d], send_sem.at[SUM], last_recv.at[y_lo, h, d], owner)

    def arrived(g, h, d, t):
        return came[g, h, at_step(h, d, t)].astype(F32)

    def sum_step(g, h, d, t):
        n = STEPS[h][d]
        owner = (z + (n - t)) % Z if d == UP else (z + Z - (n - t)) % Z
        value = own_sum(g, h, owner)
        if t > 0:
            with scope(f"rs{t - 1}{h}{d}"):
                sum_copy(g, h, d, t - 1).wait_recv()
            value += arrived(g, h, d, t - 1)
        sent[g, h, at_step(h, d, t)] = value.astype(BF16)
        go(sum_copy(g, h, d, t))

    for g in (0, 1):
        with scope(f"wt{g}"):
            got_all(weighted.at[g, pl.ds(0, PLANE - 1)], wt_recv.at[g])
        for h in range(PARTS):
            with scope(f"O{g}{h}"):
                for first in range(spans[h].start, spans[h].stop, tile):
                    size = min(tile, spans[h].stop - first)
                    value = jnp.dot(
                        weighted[g].reshape(group, 4 * count),
                        proj[:, :, :, first : first + size].reshape(4 * count, size),
                        preferred_element_type=F32,
                    )
                    result[g, :, :, first : first + size] = value.reshape(Z, rows, size)
            for d in (UP, DOWN):
                sum_step(g, h, d, 0)
    final[1 - y_lo] = result[1 - y_lo, z].astype(BF16)
    own_share = go(remote(final.at[1 - y_lo], across_share, send_sem.at[END], end_recv.at[0], across))
    order = [(g, h, t) for t in (1, 2, 3) for g in (0, 1) for h in range(PARTS)]
    for g, h, t in order:
        for d in (UP, DOWN):
            if t < STEPS[h][d]:
                sum_step(g, h, d, t)
    with scope("share"):
        own_share.wait_recv()
        sent_all(final.at[0], send_sem.at[END])
    ends = []
    for h in range(PARTS):
        for side, value in ((y_lo, result[y_lo, z, :, spans[h]]), (1 - y_lo, across_share[:, spans[h]].astype(F32))):
            for d in (UP, DOWN):
                here = last.at[side, h, d]
                with scope(f"last{h}{d}"):
                    remote(here, here, send_sem.at[SUM], last_recv.at[side, h, d], mate).wait_recv()
                value += last[side, h, d].astype(F32)
            final[side, :, spans[h]] = value.astype(BF16)
            ends.append(
                pltpu.make_async_copy(
                    final.at[side, :, spans[h]], out_ref.at[:, columns_of(side, h * width, width)],
                    local_sem.at[2 * h + len(ends) % 2],
                )
            )
            ends[-1].start()
    with scope("ends"):
        for copy in ends:
            copy.wait()
    with scope("drain"):
        sent_all(bands.at[:, pl.ds(0, Z - 1)], send_sem.at[RING])
        sent_all(away, send_sem.at[ACROSS])
        sent_all(proj.at[0, 0], send_sem.at[PIECE_SEND])
        sent_all(proj.at[0, 0], send_sem.at[MATE])
        sent_all(coefs.at[pl.ds(0, 3)], send_sem.at[COEFS])
        sent_all(proj.at[0, 0], send_sem.at[PASS])
        sent_all(parts, send_sem.at[PART])
        sent_all(weighted.at[:, pl.ds(0, PLANE - 1)], send_sem.at[WEIGHTED])
        sent_all(bands.at[:, pl.ds(0, Z - 1)], send_sem.at[SUM])


def shards(wave_rows, projectors, dij_table, dij_index, proj_count):
    rows, width = wave_rows.shape
    count = projectors.shape[0]
    half = width // 2
    kinds, per_atom, _ = dij_table.shape
    atoms = count // per_atom

    dma = pltpu.SemaphoreType.DMA
    others = PLANE - 1
    hbm = pl.BlockSpec(memory_space=pltpu.MemorySpace.HBM)
    return pl.pallas_call(
        kernel,
        out_shape=jax.ShapeDtypeStruct((rows, width), BF16),
        in_specs=[hbm] * 5,
        out_specs=pl.BlockSpec(memory_space=pl.ANY),
        scratch_shapes=[
            pltpu.VMEM((2, Z, rows, half), BF16),
            pltpu.VMEM((rows, half), BF16),
            pltpu.VMEM((2, 2, count, half), BF16),
            pltpu.VMEM((per_atom, per_atom, kinds), F32),
            pltpu.SMEM((atoms,), jnp.int32),
            pltpu.SMEM((atoms,), jnp.int32),
            pltpu.VMEM((4, per_atom, count), F32),
            pltpu.VMEM((2, PLANE, rows // 2, 4 * count), F32),
            pltpu.VMEM((2, others, rows // 2, 4 * count), F32),
            pltpu.VMEM((2, PLANE, rows // 2, 4 * count), BF16),
            pltpu.VMEM((2, Z, rows, half), F32),
            pltpu.VMEM((2, PARTS, Z - 1, rows, half // PARTS), BF16),
            pltpu.VMEM((2, PARTS, Z - 1, rows, half // PARTS), BF16),
            pltpu.VMEM((2, PARTS, 2, rows, half // PARTS), BF16),
            pltpu.VMEM((rows, half), BF16),
            pltpu.VMEM((2, rows, half), BF16),
            pltpu.VMEM((4, count, count), F32),
            dma((SENDS,)),
            dma((2, 2, Z - 1)),
            dma((2,)),
            dma((1,)),
            dma((3,)),
            dma((len(PIECES),)),
            dma((len(PIECES),)),
            dma((2,)),
            dma((2,)),
            dma((2, PARTS, Z - 3)),
            dma((2, PARTS, 2)),
            dma((1,)),
            dma((2 * PARTS,)),
        ],
        compiler_params=pltpu.CompilerParams(
            collective_id=0, has_side_effects=True, vmem_limit_bytes=67_043_328
        ),
        name="nonlocal_rows",
    )(wave_rows, projectors, jnp.transpose(dij_table, (1, 2, 0)), dij_index, proj_count)


def solution(mesh):
    return jax.shard_map(
        shards,
        mesh=mesh,
        in_specs=(P("atom", "band"), P("atom", "band"), P(), P("atom"), P("atom")),
        out_specs=P("atom", "band"),
        check_vma=False,
    )
```

```python
import functools

import jax
import jax.numpy as jnp
from jax import lax
from jax.experimental import pallas as pl
from jax.experimental.pallas import tpu as pltpu
from jax.sharding import PartitionSpec as P

MESH = pl.DeviceIdType.MESH
F32 = jnp.float32
BF16 = jnp.bfloat16
scope = jax.named_scope
Z = 8
SIDE = 4
PLANE = SIDE * SIDE
PARTS = 4
PIECES = (1024, 1024, 1024, 768, 256)
UP, DOWN = 0, 1
RING, ACROSS, HAND, PIECE_SEND, MATE, COEFS, PASS, PART, WEIGHTED, SUM, END = range(11)
SENDS = 11
STEPS = ((4, 3), (3, 4), (4, 3), (3, 4))


def kernel(
    wave_ref, proj_ref, table_ref, index_ref, count_ref, out_ref,
    bands, away, stage, proj, table, index, acting, coefs, part, parts, weighted, result, sent, came, last, across_share, final, mix,
    send_sem, ring_recv, y_recv, mate_recv, c_recv, hand_recv, piece_recv, pass_recv, part_recv, wt_recv, sum_recv, last_recv, end_recv,
    local_sem,
):
    rows, half = away.shape
    count = proj.shape[2]
    per_atom, _, kinds = table.shape
    share = rows // 2
    atom, band = lax.axis_index("atom"), lax.axis_index("band")
    y_lo, z, core = atom // (2 * Z), (atom // 2) % Z, atom % 2
    y_hi, x = band // SIDE, band % SIDE
    y = y_hi * 2 + y_lo
    me = y * SIDE + x
    slot = y_lo * 2 + core

    def at(lo, zz, cc, hi=y_hi, xx=x):
        return (lo * (2 * Z) + zz * 2 + cc, hi * SIDE + xx)

    mate = at(y_lo, z, 1 - core)
    across = at(1 - y_lo, z, core)
    corner = at(1 - y_lo, z, 1 - core)
    z_next = (at(y_lo, (z + 1) % Z, core), at(y_lo, (z + Z - 1) % Z, core))
    shifts = [(dy, dx) for dy in range(SIDE) for dx in range(SIDE) if dy or dx]
    shifts.sort(key=lambda s: -min(s[0], SIDE - s[0]) - min(s[1], SIDE - s[1]))

    def plane(dy, dx):
        yy, xx = (y + dy) % SIDE, (x + dx) % SIDE
        return yy * SIDE + xx, at(yy % 2, z, core, yy // 2, xx)

    def remote(src, dst, send, recv, to):
        return pltpu.make_async_remote_copy(
            src_ref=src, dst_ref=dst, send_sem=send, recv_sem=recv, device_id=to, device_id_type=MESH
        )

    def columns_of(side, first, size):
        return pl.ds(pl.multiple_of(side * half + first, 128), size)

    mine, theirs = columns_of(y_lo, 0, half), columns_of(1 - y_lo, 0, half)
    away_bands = pltpu.make_async_copy(wave_ref.at[:, theirs], away, local_sem.at[0])
    own_bands = pltpu.make_async_copy(wave_ref.at[:, mine], bands.at[y_lo, z], local_sem.at[1])
    own_proj = pltpu.make_async_copy(proj_ref.at[:, mine], proj.at[y_lo, core], local_sem.at[2])
    small = [
        pltpu.make_async_copy(table_ref, table, local_sem.at[3]),
        pltpu.make_async_copy(index_ref, index, local_sem.at[4]),
        pltpu.make_async_copy(count_ref, acting, local_sem.at[5]),
    ]
    for copy in (away_bands, own_bands, own_proj, *small):
        copy.start()

    barrier = pltpu.get_barrier_semaphore()
    slant = (at(1 - y_lo, (z + 1) % Z, core), at(1 - y_lo, (z + Z - 1) % Z, core))
    greet = [mate, corner, *z_next, *slant] + [plane(*s)[1] for s in shifts]
    for to in greet:
        pl.semaphore_signal(barrier, inc=1, device_id=to, device_id_type=MESH)
    with scope("barrier"):
        pl.semaphore_wait(barrier, len(greet))

    def go(copy):
        copy.start()
        return copy

    def sent_all(ref, sem):
        remote(ref, ref, sem, sem, mate).wait_send()

    def got_all(ref, sem):
        remote(ref, ref, sem, sem, mate).wait_recv()

    def ring_copy(k, h, d, t):
        source = (z + Z - t) % Z if d == UP else (z + t) % Z
        block = bands.at[y_lo if k == 0 else 1 - y_lo, source, :, pl.ds(h * (half // 2), half // 2)]
        return remote(block, block, send_sem.at[RING], ring_recv.at[k, h, d * STEPS[h][UP] + t], z_next[d])

    away_bands.wait()
    y_bands = []
    for h in (0, 1):
        columns = pl.ds(h * (half // 2), half // 2)
        y_bands.append(
            go(remote(away.at[:, columns], bands.at[y_lo, z, :, columns], send_sem.at[ACROSS], y_recv.at[h], across))
        )
    own_bands.wait()
    for h in (0, 1):
        for d in (UP, DOWN):
            go(ring_copy(0, h, d, 0))
    cuts = [(sum(PIECES[:i]), size) for i, size in enumerate(PIECES)]
    hand = remote(proj_ref.at[:, theirs], stage, send_sem.at[HAND], hand_recv.at[0], mate)
    pieces = [
        [
            remote(
                source, proj.at[y_lo, c, :, pl.ds(first, size)], send_sem.at[PIECE_SEND], piece_recv.at[c, i], across
            )
            for c, source in (
                (0, stage.at[:, pl.ds(first, size)]), (1, proj_ref.at[:, columns_of(1 - y_lo, first, size)])
            )
        ]
        for i, (first, size) in enumerate(cuts)
    ]

    @pl.when(core == 0)
    def _():
        hand.start()

    @pl.when(core == 1)
    def _():
        for i in (0, 1):
            pieces[i][1].start()

    own_proj.wait()
    there = proj.at[y_lo, core]
    to_mate = go(remote(there, there, send_sem.at[MATE], mate_recv.at[0], mate))

    for copy in small:
        copy.wait()
    flat = (per_atom, count)
    lane = lax.broadcasted_iota(jnp.int32, flat, 1)
    inner = lane % per_atom
    chosen = jnp.zeros(flat, jnp.int32)
    limit = jnp.zeros(flat, jnp.int32)
    for a in range(count // per_atom):
        chosen = jnp.where(lane // per_atom == a, index[a], chosen)
        limit = jnp.where(lane // per_atom == a, acting[a], limit)
    kind = lax.broadcasted_iota(jnp.int32, (kinds, count), 0)
    value = jnp.zeros(flat, F32)
    for i in range(per_atom):
        pick = jnp.where((kind == chosen[:1]) & (inner[:1] == i), 1.0, 0.0).astype(F32)
        value += jnp.dot(table[i], pick, precision=lax.Precision.HIGHEST, preferred_element_type=F32)
    on = (inner < limit) & (lax.broadcasted_iota(jnp.int32, flat, 0) < limit)
    coefs[slot] = jnp.where(on, value, 0.0)

    coef_copies = [
        go(remote(coefs.at[slot], coefs.at[slot], send_sem.at[COEFS], c_recv.at[i], to))
        for i, to in enumerate((mate, across, corner))
    ]
    for h in (0, 1):
        with scope(f"ybands{h}"):
            y_bands[h].wait_recv()
        for d in (UP, DOWN):
            go(ring_copy(1, h, d, 0))

    @pl.when(core == 1)
    def _():
        hand.wait_recv()
        for i in (0, 1):
            pieces[i][0].start()
        for pair in pieces[2:]:
            for copy in pair:
                copy.start()

    def passing(i):
        first, size = cuts[i]
        there = proj.at[1 - y_lo, :, :, pl.ds(first, size)]
        return remote(there, there, send_sem.at[PASS], pass_recv.at[i], mate)

    def pass_piece(i):
        @pl.when(core == 1)
        def _():
            with scope(f"piece{i}"):
                for copy in pieces[i]:
                    copy.wait_recv()
            passing(i).start()

    def take_piece(i):
        @pl.when(core == 0)
        def _():
            with scope(f"take{i}"):
                passing(i).wait_recv()

    def contract(lines, kept):
        return lax.dot_general(lines, kept, (((1,), (1,)), ((), ())), preferred_element_type=F32)

    own_pair = pl.ds(pl.multiple_of(y_lo * 2 * count, count), 2 * count)
    far_pair = pl.ds(pl.multiple_of((1 - y_lo) * 2 * count, count), 2 * count)

    def own_parts(sources):
        lines = [bands[:, source].reshape(2 * rows, half) for source in sources]
        kept = proj[y_lo].reshape(2 * count, half)
        value = contract(kept, lines[0]).T if len(lines) == 1 else contract(jnp.concatenate(lines, axis=0), kept)
        for i, source in enumerate(sources):
            here = value[i * 2 * rows : (i + 1) * 2 * rows].reshape(2, 2, share, 2 * count)
            part[:, pl.ds(source * 2, 2), :, own_pair] = here

    def send_parts(g, columns):
        for i, s in enumerate(shifts):
            chunk, to = plane(*s)
            go(
                remote(
                    part.at[g, chunk, :, columns], parts.at[g, i, :, columns], send_sem.at[PART], part_recv.at[g], to
                )
            )

    for t in range(4):
        for k in (0, 1):
            for h in (0, 1):
                for d in (UP, DOWN):
                    if t < STEPS[h][d]:
                        with scope(f"ag{t}{k}{h}{d}"):
                            ring_copy(k, h, d, t).wait_recv()
                        if t + 1 < STEPS[h][d]:
                            go(ring_copy(k, h, d, t + 1))
        if t == 1:
            pass_piece(0)
            with scope("tomate"):
                to_mate.wait_recv()
            with scope("S1"):
                own_parts([(z + Z + i) % Z for i in range(-2, 3)])
        if t == 2:
            pass_piece(1)
            with scope("S2"):
                own_parts([(z + Z - 3) % Z, (z + 3) % Z])
            pass_piece(2)
    with scope("S3"):
        own_parts([(z + 4) % Z])
    every = 2 * Z * rows

    def far_parts(first, size):
        return contract(
            bands[:, :, :, first : first + size].reshape(every, size),
            proj[1 - y_lo, :, :, first : first + size].reshape(2 * count, size),
        ).reshape(2, PLANE, share, 2 * count)

    for i in range(3):
        take_piece(i)
    with scope("Sfar0"):
        part[:, :, :, far_pair] = far_parts(0, cuts[3][0])
    pass_piece(3)
    take_piece(3)
    with scope("Sfar1"):
        part[:, :, :, far_pair] += far_parts(*cuts[3])
    pass_piece(4)
    with scope("mixes"):
        for copy in coef_copies:
            copy.wait_recv()
        square = (count, count)
        down = lax.broadcasted_iota(jnp.int32, square, 0)
        same = down // per_atom == lax.broadcasted_iota(jnp.int32, square, 1) // per_atom
        for s in range(4):
            mix[s] = jnp.where(same, jnp.concatenate([coefs[s]] * (count // per_atom), axis=0), 0.0)
    take_piece(4)
    with scope("Sfar2"):
        part[:, :, :, far_pair] += far_parts(*cuts[4])
    for g in (0, 1):
        send_parts(g, slice(None))
    for g in (0, 1):
        with scope(f"part{g}"):
            got_all(parts.at[g], part_recv.at[g])
        with scope(f"mix{g}"):
            total = part[g, me]
            for i in range(len(shifts)):
                total += parts[g, i]
            mixed = [
                jnp.dot(
                    total[:, s * count : (s + 1) * count], mix[s],
                    precision=lax.Precision.HIGHEST, preferred_element_type=F32,
                )
                for s in range(4)
            ]
            weighted[g, me] = jnp.concatenate(mixed, axis=1).astype(BF16)
        for i, s in enumerate(shifts):
            _, to = plane(*s)
            there = weighted.at[g, me]
            go(remote(there, there, send_sem.at[WEIGHTED], wt_recv.at[g], to))

    group = Z * rows
    tile = 512
    width = half // PARTS
    spans = [slice(h * width, (h + 1) * width) for h in range(PARTS)]

    def own_sum(g, h, owner):
        return result[g, owner, :, spans[h]]

    def at_step(h, d, t):
        return d * STEPS[h][UP] + t

    def sum_copy(g, h, d, t):
        n = at_step(h, d, t)
        if t < STEPS[h][d] - 1:
            return remote(
                sent.at[g, h, n], came.at[g, h, n], send_sem.at[SUM], sum_recv.at[g, h, n - d], z_next[d]
            )
        owner = at(g, (z + 1) % Z if d == UP else (z + Z - 1) % Z, core)
        return remote(sent.at[g, h, n], last.at[y_lo, h, d], send_sem.at[SUM], last_recv.at[y_lo, h, d], owner)

    def arrived(g, h, d, t):
        return came[g, h, at_step(h, d, t)].astype(F32)

    def sum_step(g, h, d, t):
        n = STEPS[h][d]
        owner = (z + (n - t)) % Z if d == UP else (z + Z - (n - t)) % Z
        value = own_sum(g, h, owner)
        if t > 0:
            with scope(f"rs{t - 1}{h}{d}"):
                sum_copy(g, h, d, t - 1).wait_recv()
            value += arrived(g, h, d, t - 1)
        sent[g, h, at_step(h, d, t)] = value.astype(BF16)
        go(sum_copy(g, h, d, t))

    for g in (0, 1):
        with scope(f"wt{g}"):
            got_all(weighted.at[g, pl.ds(0, PLANE - 1)], wt_recv.at[g])
        for h in range(PARTS):
            with scope(f"O{g}{h}"):
                for first in range(spans[h].start, spans[h].stop, tile):
                    size = min(tile, spans[h].stop - first)
                    value = jnp.dot(
                        weighted[g].reshape(group, 4 * count),
                        proj[:, :, :, first : first + size].reshape(4 * count, size),
                        preferred_element_type=F32,
                    )
                    result[g, :, :, first : first + size] = value.reshape(Z, rows, size)
            for d in (UP, DOWN):
                sum_step(g, h, d, 0)
    final[1 - y_lo] = result[1 - y_lo, z].astype(BF16)
    own_share = go(remote(final.at[1 - y_lo], across_share, send_sem.at[END], end_recv.at[0], across))
    order = [(g, h, t) for t in (1, 2, 3) for g in (0, 1) for h in range(PARTS)]
    for g, h, t in order:
        for d in (UP, DOWN):
            if t < STEPS[h][d]:
                sum_step(g, h, d, t)
    with scope("share"):
        own_share.wait_recv()
        sent_all(final.at[0], send_sem.at[END])
    ends = []
    for h in range(PARTS):
        for side, value in ((y_lo, result[y_lo, z, :, spans[h]]), (1 - y_lo, across_share[:, spans[h]].astype(F32))):
            for d in (UP, DOWN):
                here = last.at[side, h, d]
                with scope(f"last{h}{d}"):
                    remote(here, here, send_sem.at[SUM], last_recv.at[side, h, d], mate).wait_recv()
                value += last[side, h, d].astype(F32)
            final[side, :, spans[h]] = value.astype(BF16)
            ends.append(
                pltpu.make_async_copy(
                    final.at[side, :, spans[h]], out_ref.at[:, columns_of(side, h * width, width)],
                    local_sem.at[2 * h + len(ends) % 2],
                )
            )
            ends[-1].start()
    with scope("ends"):
        for copy in ends:
            copy.wait()
    with scope("drain"):
        sent_all(bands.at[:, pl.ds(0, Z - 1)], send_sem.at[RING])
        sent_all(away, send_sem.at[ACROSS])
        sent_all(proj.at[0, 0], send_sem.at[MATE])
        sent_all(coefs.at[pl.ds(0, 3)], send_sem.at[COEFS])

        @pl.when(core == 0)
        def _():
            sent_all(stage, send_sem.at[HAND])

        @pl.when(core == 1)
        def _():
            sent_all(proj.at[0], send_sem.at[PIECE_SEND])
            sent_all(proj.at[0], send_sem.at[PASS])

        sent_all(parts, send_sem.at[PART])
        sent_all(weighted.at[:, pl.ds(0, PLANE - 1)], send_sem.at[WEIGHTED])
        sent_all(bands.at[:, pl.ds(0, Z - 1)], send_sem.at[SUM])


def shards(wave_rows, projectors, dij_table, dij_index, proj_count):
    rows, width = wave_rows.shape
    count = projectors.shape[0]
    half = width // 2
    kinds, per_atom, _ = dij_table.shape
    atoms = count // per_atom

    dma = pltpu.SemaphoreType.DMA
    others = PLANE - 1
    hbm = pl.BlockSpec(memory_space=pltpu.MemorySpace.HBM)
    return pl.pallas_call(
        kernel,
        out_shape=jax.ShapeDtypeStruct((rows, width), BF16),
        in_specs=[hbm] * 5,
        out_specs=pl.BlockSpec(memory_space=pl.ANY),
        scratch_shapes=[
            pltpu.VMEM((2, Z, rows, half), BF16),
            pltpu.VMEM((rows, half), BF16),
            pltpu.VMEM((count, half), BF16),
            pltpu.VMEM((2, 2, count, half), BF16),
            pltpu.VMEM((per_atom, per_atom, kinds), F32),
            pltpu.SMEM((atoms,), jnp.int32),
            pltpu.SMEM((atoms,), jnp.int32),
            pltpu.VMEM((4, per_atom, count), F32),
            pltpu.VMEM((2, PLANE, rows // 2, 4 * count), F32),
            pltpu.VMEM((2, others, rows // 2, 4 * count), F32),
            pltpu.VMEM((2, PLANE, rows // 2, 4 * count), BF16),
            pltpu.VMEM((2, Z, rows, half), F32),
            pltpu.VMEM((2, PARTS, Z - 1, rows, half // PARTS), BF16),
            pltpu.VMEM((2, PARTS, Z - 1, rows, half // PARTS), BF16),
            pltpu.VMEM((2, PARTS, 2, rows, half // PARTS), BF16),
            pltpu.VMEM((rows, half), BF16),
            pltpu.VMEM((2, rows, half), BF16),
            pltpu.VMEM((4, count, count), F32),
            dma((SENDS,)),
            dma((2, 2, Z - 1)),
            dma((2,)),
            dma((1,)),
            dma((3,)),
            dma((1,)),
            dma((2, len(PIECES))),
            dma((len(PIECES),)),
            dma((2,)),
            dma((2,)),
            dma((2, PARTS, Z - 3)),
            dma((2, PARTS, 2)),
            dma((1,)),
            dma((2 * PARTS,)),
        ],
        compiler_params=pltpu.CompilerParams(
            collective_id=0, has_side_effects=True, vmem_limit_bytes=67_043_328
        ),
        name="nonlocal_rows",
    )(wave_rows, projectors, jnp.transpose(dij_table, (1, 2, 0)), dij_index, proj_count)


def solution(mesh):
    return jax.shard_map(
        shards,
        mesh=mesh,
        in_specs=(P("atom", "band"), P("atom", "band"), P(), P("atom"), P("atom")),
        out_specs=P("atom", "band"),
        check_vma=False,
    )
```

```python
import functools

import jax
import jax.numpy as jnp
from jax import lax
from jax.experimental import pallas as pl
from jax.experimental.pallas import tpu as pltpu
from jax.sharding import PartitionSpec as P

MESH = pl.DeviceIdType.MESH
F32 = jnp.float32
BF16 = jnp.bfloat16
scope = jax.named_scope
Z = 8
SIDE = 4
PLANE = SIDE * SIDE
PARTS = 4
PIECES = (1024, 1024, 1024, 768, 256)
UP, DOWN = 0, 1
RING, ACROSS, HAND, PIECE_SEND, MATE, COEFS, PASS, PART, WEIGHTED, SUM, END = range(11)
SENDS = 11
STEPS = ((4, 3), (3, 4), (4, 3), (3, 4))


def kernel(
    wave_ref, proj_ref, table_ref, index_ref, count_ref, out_ref,
    bands, away, stage, proj, table, index, acting, coefs, part, parts, weighted, result, sent, came, last, across_share, final, mix,
    send_sem, ring_recv, y_recv, mate_recv, c_recv, hand_recv, piece_recv, pass_recv, part_recv, wt_recv, sum_recv, last_recv, end_recv,
    local_sem,
):
    rows, half = away.shape
    count = proj.shape[2]
    per_atom, _, kinds = table.shape
    share = rows // 2
    atom, band = lax.axis_index("atom"), lax.axis_index("band")
    y_lo, z, core = atom // (2 * Z), (atom // 2) % Z, atom % 2
    y_hi, x = band // SIDE, band % SIDE
    y = y_hi * 2 + y_lo
    me = y * SIDE + x
    slot = y_lo * 2 + core

    def at(lo, zz, cc, hi=y_hi, xx=x):
        return (lo * (2 * Z) + zz * 2 + cc, hi * SIDE + xx)

    mate = at(y_lo, z, 1 - core)
    across = at(1 - y_lo, z, core)
    corner = at(1 - y_lo, z, 1 - core)
    z_next = (at(y_lo, (z + 1) % Z, core), at(y_lo, (z + Z - 1) % Z, core))
    shifts = [(dy, dx) for dy in range(SIDE) for dx in range(SIDE) if dy or dx]
    shifts.sort(key=lambda s: -min(s[0], SIDE - s[0]) - min(s[1], SIDE - s[1]))

    def plane(dy, dx):
        yy, xx = (y + dy) % SIDE, (x + dx) % SIDE
        return yy * SIDE + xx, at(yy % 2, z, core, yy // 2, xx)

    def remote(src, dst, send, recv, to):
        return pltpu.make_async_remote_copy(
            src_ref=src, dst_ref=dst, send_sem=send, recv_sem=recv, device_id=to, device_id_type=MESH
        )

    def columns_of(side, first, size):
        return pl.ds(pl.multiple_of(side * half + first, 128), size)

    mine, theirs = columns_of(y_lo, 0, half), columns_of(1 - y_lo, 0, half)
    away_bands = pltpu.make_async_copy(wave_ref.at[:, theirs], away, local_sem.at[0])
    own_bands = pltpu.make_async_copy(wave_ref.at[:, mine], bands.at[y_lo, z], local_sem.at[1])
    own_proj = pltpu.make_async_copy(proj_ref.at[:, mine], proj.at[y_lo, core], local_sem.at[2])
    small = [
        pltpu.make_async_copy(table_ref, table, local_sem.at[3]),
        pltpu.make_async_copy(index_ref, index, local_sem.at[4]),
        pltpu.make_async_copy(count_ref, acting, local_sem.at[5]),
    ]
    for copy in (away_bands, own_bands, own_proj, *small):
        copy.start()

    barrier = pltpu.get_barrier_semaphore()
    slant = (at(1 - y_lo, (z + 1) % Z, core), at(1 - y_lo, (z + Z - 1) % Z, core))
    greet = [mate, corner, *z_next, *slant] + [plane(*s)[1] for s in shifts]
    for to in greet:
        pl.semaphore_signal(barrier, inc=1, device_id=to, device_id_type=MESH)
    with scope("barrier"):
        pl.semaphore_wait(barrier, len(greet))

    def go(copy):
        copy.start()
        return copy

    def sent_all(ref, sem):
        remote(ref, ref, sem, sem, mate).wait_send()

    def got_all(ref, sem):
        remote(ref, ref, sem, sem, mate).wait_recv()

    def ring_copy(k, h, d, t):
        source = (z + Z - t) % Z if d == UP else (z + t) % Z
        block = bands.at[y_lo if k == 0 else 1 - y_lo, source, :, pl.ds(h * (half // 2), half // 2)]
        return remote(block, block, send_sem.at[RING], ring_recv.at[k, h, d * STEPS[h][UP] + t], z_next[d])

    away_bands.wait()
    y_bands = []
    for h in (0, 1):
        columns = pl.ds(h * (half // 2), half // 2)
        y_bands.append(
            go(remote(away.at[:, columns], bands.at[y_lo, z, :, columns], send_sem.at[ACROSS], y_recv.at[h], across))
        )
    own_bands.wait()
    for h in (0, 1):
        for d in (UP, DOWN):
            go(ring_copy(0, h, d, 0))
    cuts = [(sum(PIECES[:i]), size) for i, size in enumerate(PIECES)]
    hand = remote(proj_ref.at[:, theirs], stage, send_sem.at[HAND], hand_recv.at[0], mate)
    pieces = [
        [
            remote(
                source, proj.at[y_lo, c, :, pl.ds(first, size)], send_sem.at[PIECE_SEND], piece_recv.at[c, i], across
            )
            for c, source in (
                (0, stage.at[:, pl.ds(first, size)]), (1, proj_ref.at[:, columns_of(1 - y_lo, first, size)])
            )
        ]
        for i, (first, size) in enumerate(cuts)
    ]

    @pl.when(core == 0)
    def _():
        hand.start()

    @pl.when(core == 1)
    def _():
        for i in (0, 1):
            pieces[i][1].start()

    own_proj.wait()
    there = proj.at[y_lo, core]
    to_mate = go(remote(there, there, send_sem.at[MATE], mate_recv.at[0], mate))

    for copy in small:
        copy.wait()
    flat = (per_atom, count)
    lane = lax.broadcasted_iota(jnp.int32, flat, 1)
    inner = lane % per_atom
    chosen = jnp.zeros(flat, jnp.int32)
    limit = jnp.zeros(flat, jnp.int32)
    for a in range(count // per_atom):
        chosen = jnp.where(lane // per_atom == a, index[a], chosen)
        limit = jnp.where(lane // per_atom == a, acting[a], limit)
    kind = lax.broadcasted_iota(jnp.int32, (kinds, count), 0)
    value = jnp.zeros(flat, F32)
    for i in range(per_atom):
        pick = jnp.where((kind == chosen[:1]) & (inner[:1] == i), 1.0, 0.0).astype(F32)
        value += jnp.dot(table[i], pick, precision=lax.Precision.HIGHEST, preferred_element_type=F32)
    on = (inner < limit) & (lax.broadcasted_iota(jnp.int32, flat, 0) < limit)
    coefs[slot] = jnp.where(on, value, 0.0)

    coef_copies = [
        go(remote(coefs.at[slot], coefs.at[slot], send_sem.at[COEFS], c_recv.at[i], to))
        for i, to in enumerate((mate, across, corner))
    ]
    for h in (0, 1):
        with scope(f"ybands{h}"):
            y_bands[h].wait_recv()
        for d in (UP, DOWN):
            go(ring_copy(1, h, d, 0))

    @pl.when(core == 1)
    def _():
        hand.wait_recv()
        for i in (0, 1):
            pieces[i][0].start()
        for pair in pieces[2:]:
            for copy in pair:
                copy.start()

    def passing(i):
        first, size = cuts[i]
        there = proj.at[1 - y_lo, :, :, pl.ds(first, size)]
        return remote(there, there, send_sem.at[PASS], pass_recv.at[i], mate)

    def pass_piece(i):
        @pl.when(core == 1)
        def _():
            with scope(f"piece{i}"):
                for copy in pieces[i]:
                    copy.wait_recv()
            passing(i).start()

    def take_piece(i):
        @pl.when(core == 0)
        def _():
            with scope(f"take{i}"):
                passing(i).wait_recv()

    def contract(lines, kept):
        return lax.dot_general(lines, kept, (((1,), (1,)), ((), ())), preferred_element_type=F32)

    own_pair = pl.ds(pl.multiple_of(y_lo * 2 * count, count), 2 * count)
    far_pair = pl.ds(pl.multiple_of((1 - y_lo) * 2 * count, count), 2 * count)

    def own_parts(sources):
        lines = [bands[:, source].reshape(2 * rows, half) for source in sources]
        kept = proj[y_lo].reshape(2 * count, half)
        value = contract(kept, lines[0]).T if len(lines) == 1 else contract(jnp.concatenate(lines, axis=0), kept)
        for i, source in enumerate(sources):
            here = value[i * 2 * rows : (i + 1) * 2 * rows].reshape(2, 2, share, 2 * count)
            part[:, pl.ds(source * 2, 2), :, own_pair] = here

    def send_parts(g, columns):
        for i, s in enumerate(shifts):
            chunk, to = plane(*s)
            go(
                remote(
                    part.at[g, chunk, :, columns], parts.at[g, i, :, columns], send_sem.at[PART], part_recv.at[g], to
                )
            )

    for t in range(4):
        for k in (0, 1):
            for h in (0, 1):
                for d in (UP, DOWN):
                    if t < STEPS[h][d]:
                        with scope(f"ag{t}{k}{h}{d}"):
                            ring_copy(k, h, d, t).wait_recv()
                        if t + 1 < STEPS[h][d]:
                            go(ring_copy(k, h, d, t + 1))
        if t == 1:
            pass_piece(0)
            with scope("tomate"):
                to_mate.wait_recv()
            with scope("S1"):
                own_parts([(z + Z + i) % Z for i in range(-2, 3)])
        if t == 2:
            pass_piece(1)
            with scope("S2"):
                own_parts([(z + Z - 3) % Z, (z + 3) % Z])
            pass_piece(2)
    with scope("S3"):
        own_parts([(z + 4) % Z])
    every = 2 * Z * rows

    def far_parts(first, size):
        return contract(
            bands[:, :, :, first : first + size].reshape(every, size),
            proj[1 - y_lo, :, :, first : first + size].reshape(2 * count, size),
        ).reshape(2, PLANE, share, 2 * count)

    for i in range(3):
        take_piece(i)
    with scope("Sfar0"):
        part[:, :, :, far_pair] = far_parts(0, cuts[3][0])
    pass_piece(3)
    take_piece(3)
    with scope("Sfar1"):
        part[:, :, :, far_pair] += far_parts(*cuts[3])
    pass_piece(4)
    with scope("mixes"):
        for copy in coef_copies:
            copy.wait_recv()
        square = (count, count)
        down = lax.broadcasted_iota(jnp.int32, square, 0)
        same = down // per_atom == lax.broadcasted_iota(jnp.int32, square, 1) // per_atom
        for s in range(4):
            mix[s] = jnp.where(same, jnp.concatenate([coefs[s]] * (count // per_atom), axis=0), 0.0)
    take_piece(4)
    with scope("Sfar2"):
        part[:, :, :, far_pair] += far_parts(*cuts[4])
    for g in (0, 1):
        send_parts(g, slice(None))
    for g in (0, 1):
        with scope(f"part{g}"):
            got_all(parts.at[g], part_recv.at[g])
        with scope(f"mix{g}"):
            total = part[g, me]
            for i in range(len(shifts)):
                total += parts[g, i]
            mixed = [
                jnp.dot(
                    total[:, s * count : (s + 1) * count], mix[s],
                    precision=lax.Precision.HIGHEST, preferred_element_type=F32,
                )
                for s in range(4)
            ]
            weighted[g, me] = jnp.concatenate(mixed, axis=1).astype(BF16)
        for i, s in enumerate(shifts):
            _, to = plane(*s)
            there = weighted.at[g, me]
            go(remote(there, there, send_sem.at[WEIGHTED], wt_recv.at[g], to))

    group = Z * rows
    tile = 512
    width = half // PARTS
    spans = [slice(h * width, (h + 1) * width) for h in range(PARTS)]

    def own_sum(g, h, owner):
        return result[g, owner, :, spans[h]]

    def at_step(h, d, t):
        return d * STEPS[h][UP] + t

    def sum_copy(g, h, d, t):
        n = at_step(h, d, t)
        if t < STEPS[h][d] - 1:
            return remote(
                sent.at[g, h, n], came.at[g, h, n], send_sem.at[SUM], sum_recv.at[g, h, n - d], z_next[d]
            )
        owner = at(g, (z + 1) % Z if d == UP else (z + Z - 1) % Z, core)
        return remote(sent.at[g, h, n], last.at[y_lo, h, d], send_sem.at[SUM], last_recv.at[y_lo, h, d], owner)

    def arrived(g, h, d, t):
        return came[g, h, at_step(h, d, t)].astype(F32)

    def sum_step(g, h, d, t):
        n = STEPS[h][d]
        owner = (z + (n - t)) % Z if d == UP else (z + Z - (n - t)) % Z
        value = own_sum(g, h, owner)
        if t > 0:
            with scope(f"rs{t - 1}{h}{d}"):
                sum_copy(g, h, d, t - 1).wait_recv()
            value += arrived(g, h, d, t - 1)
        sent[g, h, at_step(h, d, t)] = value.astype(BF16)
        go(sum_copy(g, h, d, t))

    for g in (0, 1):
        with scope(f"wt{g}"):
            got_all(weighted.at[g, pl.ds(0, PLANE - 1)], wt_recv.at[g])
        for h in range(PARTS):
            with scope(f"O{g}{h}"):
                for first in range(spans[h].start, spans[h].stop, tile):
                    size = min(tile, spans[h].stop - first)
                    value = jnp.dot(
                        weighted[g].reshape(group, 4 * count),
                        proj[:, :, :, first : first + size].reshape(4 * count, size),
                        preferred_element_type=F32,
                    )
                    result[g, :, :, first : first + size] = value.reshape(Z, rows, size)
            for d in (UP, DOWN):
                sum_step(g, h, d, 0)
    final[1 - y_lo] = result[1 - y_lo, z].astype(BF16)
    own_share = go(remote(final.at[1 - y_lo], across_share, send_sem.at[END], end_recv.at[0], across))
    order = [(g, h, t) for t in (1, 2, 3) for g in (0, 1) for h in range(PARTS)]
    for g, h, t in order:
        for d in (UP, DOWN):
            if t < STEPS[h][d]:
                sum_step(g, h, d, t)
    with scope("share"):
        own_share.wait_recv()
        sent_all(final.at[0], send_sem.at[END])
    for h in range(PARTS):
        for side, value in ((y_lo, result[y_lo, z, :, spans[h]]), (1 - y_lo, across_share[:, spans[h]].astype(F32))):
            for d in (UP, DOWN):
                here = last.at[side, h, d]
                with scope(f"last{h}{d}"):
                    remote(here, here, send_sem.at[SUM], last_recv.at[side, h, d], mate).wait_recv()
                value += last[side, h, d].astype(F32)
            out_ref[:, columns_of(side, h * width, width)] = value.astype(BF16)
    with scope("drain"):
        sent_all(bands.at[:, pl.ds(0, Z - 1)], send_sem.at[RING])
        sent_all(away, send_sem.at[ACROSS])
        sent_all(proj.at[0, 0], send_sem.at[MATE])
        sent_all(coefs.at[pl.ds(0, 3)], send_sem.at[COEFS])

        @pl.when(core == 0)
        def _():
            sent_all(stage, send_sem.at[HAND])

        @pl.when(core == 1)
        def _():
            sent_all(proj.at[0], send_sem.at[PIECE_SEND])
            sent_all(proj.at[0], send_sem.at[PASS])

        sent_all(parts, send_sem.at[PART])
        sent_all(weighted.at[:, pl.ds(0, PLANE - 1)], send_sem.at[WEIGHTED])
        sent_all(bands.at[:, pl.ds(0, Z - 1)], send_sem.at[SUM])


def shards(wave_rows, projectors, dij_table, dij_index, proj_count):
    rows, width = wave_rows.shape
    count = projectors.shape[0]
    half = width // 2
    kinds, per_atom, _ = dij_table.shape
    atoms = count // per_atom

    dma = pltpu.SemaphoreType.DMA
    others = PLANE - 1
    hbm = pl.BlockSpec(memory_space=pltpu.MemorySpace.HBM)
    operands = [
        pltpu.with_memory_space_constraint(value, pltpu.MemorySpace.HBM)
        for value in (wave_rows, projectors, jnp.transpose(dij_table, (1, 2, 0)), dij_index, proj_count)
    ]
    return pl.pallas_call(
        kernel,
        out_shape=jax.ShapeDtypeStruct((rows, width), BF16),
        in_specs=[hbm] * 5,
        out_specs=pl.BlockSpec(memory_space=pltpu.MemorySpace.VMEM),
        scratch_shapes=[
            pltpu.VMEM((2, Z, rows, half), BF16),
            pltpu.VMEM((rows, half), BF16),
            pltpu.VMEM((count, half), BF16),
            pltpu.VMEM((2, 2, count, half), BF16),
            pltpu.VMEM((per_atom, per_atom, kinds), F32),
            pltpu.SMEM((atoms,), jnp.int32),
            pltpu.SMEM((atoms,), jnp.int32),
            pltpu.VMEM((4, per_atom, count), F32),
            pltpu.VMEM((2, PLANE, rows // 2, 4 * count), F32),
            pltpu.VMEM((2, others, rows // 2, 4 * count), F32),
            pltpu.VMEM((2, PLANE, rows // 2, 4 * count), BF16),
            pltpu.VMEM((2, Z, rows, half), F32),
            pltpu.VMEM((2, PARTS, Z - 1, rows, half // PARTS), BF16),
            pltpu.VMEM((2, PARTS, Z - 1, rows, half // PARTS), BF16),
            pltpu.VMEM((2, PARTS, 2, rows, half // PARTS), BF16),
            pltpu.VMEM((rows, half), BF16),
            pltpu.VMEM((2, rows, half), BF16),
            pltpu.VMEM((4, count, count), F32),
            dma((SENDS,)),
            dma((2, 2, Z - 1)),
            dma((2,)),
            dma((1,)),
            dma((3,)),
            dma((1,)),
            dma((2, len(PIECES))),
            dma((len(PIECES),)),
            dma((2,)),
            dma((2,)),
            dma((2, PARTS, Z - 3)),
            dma((2, PARTS, 2)),
            dma((1,)),
            dma((2 * PARTS,)),
        ],
        compiler_params=pltpu.CompilerParams(
            collective_id=0, has_side_effects=True, vmem_limit_bytes=40 * 1024 * 1024
        ),
        name="nonlocal_rows",
    )(*operands)


def solution(mesh):
    return jax.shard_map(
        shards,
        mesh=mesh,
        in_specs=(P("atom", "band"), P("atom", "band"), P(), P("atom"), P("atom")),
        out_specs=P("atom", "band"),
        check_vma=False,
    )
```

```python
import functools

import jax
import jax.numpy as jnp
from jax import lax
from jax.experimental import pallas as pl
from jax.experimental.pallas import tpu as pltpu
from jax.sharding import PartitionSpec as P

MESH = pl.DeviceIdType.MESH
F32 = jnp.float32
BF16 = jnp.bfloat16
scope = jax.named_scope
Z = 8
SIDE = 4
PLANE = SIDE * SIDE
PARTS = 4
PIECES = (1024, 1024, 1024, 896, 128)
UP, DOWN = 0, 1
RING, ACROSS, HAND, PIECE_SEND, MATE, COEFS, PASS, PART, WEIGHTED, SUM, END = range(11)
SENDS = 11
STEPS = ((4, 3), (3, 4), (4, 3), (3, 4))


def kernel(
    wave_ref, proj_ref, table_ref, index_ref, count_ref, out_ref,
    bands, away, stage, proj, table, index, acting, coefs, part, parts, weighted, result, sent, came, last, across_share, final, mix,
    send_sem, ring_recv, y_recv, mate_recv, c_recv, hand_recv, piece_recv, pass_recv, part_recv, wt_recv, sum_recv, last_recv, end_recv,
    local_sem,
):
    rows, half = away.shape
    count = proj.shape[2]
    per_atom, _, kinds = table.shape
    share = rows // 2
    atom, band = lax.axis_index("atom"), lax.axis_index("band")
    y_lo, z, core = atom // (2 * Z), (atom // 2) % Z, atom % 2
    y_hi, x = band // SIDE, band % SIDE
    y = y_hi * 2 + y_lo
    me = y * SIDE + x
    slot = y_lo * 2 + core

    def at(lo, zz, cc, hi=y_hi, xx=x):
        return (lo * (2 * Z) + zz * 2 + cc, hi * SIDE + xx)

    mate = at(y_lo, z, 1 - core)
    across = at(1 - y_lo, z, core)
    corner = at(1 - y_lo, z, 1 - core)
    z_next = (at(y_lo, (z + 1) % Z, core), at(y_lo, (z + Z - 1) % Z, core))
    shifts = [(dy, dx) for dy in range(SIDE) for dx in range(SIDE) if dy or dx]
    shifts.sort(key=lambda s: -2 * min(s[0], SIDE - s[0]) - min(s[1], SIDE - s[1]))

    def plane(dy, dx):
        yy, xx = (y + dy) % SIDE, (x + dx) % SIDE
        return yy * SIDE + xx, at(yy % 2, z, core, yy // 2, xx)

    def remote(src, dst, send, recv, to):
        return pltpu.make_async_remote_copy(
            src_ref=src, dst_ref=dst, send_sem=send, recv_sem=recv, device_id=to, device_id_type=MESH
        )

    def columns_of(side, first, size):
        return pl.ds(pl.multiple_of(side * half + first, 128), size)

    mine, theirs = columns_of(y_lo, 0, half), columns_of(1 - y_lo, 0, half)
    away_bands = pltpu.make_async_copy(wave_ref.at[:, theirs], away, local_sem.at[0])
    own_bands = pltpu.make_async_copy(wave_ref.at[:, mine], bands.at[y_lo, z], local_sem.at[1])
    own_proj = pltpu.make_async_copy(proj_ref.at[:, mine], proj.at[y_lo, core], local_sem.at[2])
    small = [
        pltpu.make_async_copy(table_ref, table, local_sem.at[3]),
        pltpu.make_async_copy(index_ref, index, local_sem.at[4]),
        pltpu.make_async_copy(count_ref, acting, local_sem.at[5]),
    ]
    for copy in (away_bands, own_bands, own_proj, *small):
        copy.start()

    barrier = pltpu.get_barrier_semaphore()
    slant = (at(1 - y_lo, (z + 1) % Z, core), at(1 - y_lo, (z + Z - 1) % Z, core))
    greet = [mate, corner, *z_next, *slant] + [plane(*s)[1] for s in shifts]
    for to in greet:
        pl.semaphore_signal(barrier, inc=1, device_id=to, device_id_type=MESH)
    with scope("barrier"):
        pl.semaphore_wait(barrier, len(greet))

    def go(copy):
        copy.start()
        return copy

    def sent_all(ref, sem):
        remote(ref, ref, sem, sem, mate).wait_send()

    def got_all(ref, sem):
        remote(ref, ref, sem, sem, mate).wait_recv()

    def ring_copy(k, h, d, t):
        source = (z + Z - t) % Z if d == UP else (z + t) % Z
        block = bands.at[y_lo if k == 0 else 1 - y_lo, source, :, pl.ds(h * (half // 2), half // 2)]
        return remote(block, block, send_sem.at[RING], ring_recv.at[k, h, d * STEPS[h][UP] + t], z_next[d])

    away_bands.wait()
    y_bands = []
    for h in (0, 1):
        columns = pl.ds(h * (half // 2), half // 2)
        y_bands.append(
            go(remote(away.at[:, columns], bands.at[y_lo, z, :, columns], send_sem.at[ACROSS], y_recv.at[h], across))
        )
    own_bands.wait()
    for h in (0, 1):
        for d in (UP, DOWN):
            go(ring_copy(0, h, d, 0))
    cuts = [(sum(PIECES[:i]), size) for i, size in enumerate(PIECES)]
    hand = remote(proj_ref.at[:, theirs], stage, send_sem.at[HAND], hand_recv.at[0], mate)
    pieces = [
        [
            remote(
                source, proj.at[y_lo, c, :, pl.ds(first, size)], send_sem.at[PIECE_SEND], piece_recv.at[c, i], across
            )
            for c, source in (
                (0, stage.at[:, pl.ds(first, size)]), (1, proj_ref.at[:, columns_of(1 - y_lo, first, size)])
            )
        ]
        for i, (first, size) in enumerate(cuts)
    ]

    @pl.when(core == 0)
    def _():
        hand.start()

    @pl.when(core == 1)
    def _():
        for i in (0, 1):
            pieces[i][1].start()

    own_proj.wait()
    there = proj.at[y_lo, core]
    to_mate = go(remote(there, there, send_sem.at[MATE], mate_recv.at[0], mate))

    for copy in small:
        copy.wait()
    flat = (per_atom, count)
    lane = lax.broadcasted_iota(jnp.int32, flat, 1)
    inner = lane % per_atom
    chosen = jnp.zeros(flat, jnp.int32)
    limit = jnp.zeros(flat, jnp.int32)
    for a in range(count // per_atom):
        chosen = jnp.where(lane // per_atom == a, index[a], chosen)
        limit = jnp.where(lane // per_atom == a, acting[a], limit)
    kind = lax.broadcasted_iota(jnp.int32, (kinds, count), 0)
    value = jnp.zeros(flat, F32)
    for i in range(per_atom):
        pick = jnp.where((kind == chosen[:1]) & (inner[:1] == i), 1.0, 0.0).astype(F32)
        value += jnp.dot(table[i], pick, precision=lax.Precision.HIGHEST, preferred_element_type=F32)
    on = (inner < limit) & (lax.broadcasted_iota(jnp.int32, flat, 0) < limit)
    coefs[slot] = jnp.where(on, value, 0.0)

    coef_copies = [
        go(remote(coefs.at[slot], coefs.at[slot], send_sem.at[COEFS], c_recv.at[i], to))
        for i, to in enumerate((mate, across, corner))
    ]
    for h in (0, 1):
        with scope(f"ybands{h}"):
            y_bands[h].wait_recv()
        for d in (UP, DOWN):
            go(ring_copy(1, h, d, 0))

    @pl.when(core == 1)
    def _():
        hand.wait_recv()
        for i in (0, 1):
            pieces[i][0].start()
        for pair in pieces[2:]:
            for copy in pair:
                copy.start()

    def passing(i):
        first, size = cuts[i]
        there = proj.at[1 - y_lo, :, :, pl.ds(first, size)]
        return remote(there, there, send_sem.at[PASS], pass_recv.at[i], mate)

    def pass_piece(i):
        @pl.when(core == 1)
        def _():
            with scope(f"piece{i}"):
                for copy in pieces[i]:
                    copy.wait_recv()
            passing(i).start()

    def take_piece(i):
        @pl.when(core == 0)
        def _():
            with scope(f"take{i}"):
                passing(i).wait_recv()

    def contract(lines, kept):
        return lax.dot_general(lines, kept, (((1,), (1,)), ((), ())), preferred_element_type=F32)

    own_pair = pl.ds(pl.multiple_of(y_lo * 2 * count, count), 2 * count)
    far_pair = pl.ds(pl.multiple_of((1 - y_lo) * 2 * count, count), 2 * count)

    def own_parts(sources):
        lines = [bands[:, source].reshape(2 * rows, half) for source in sources]
        kept = proj[y_lo].reshape(2 * count, half)
        value = contract(kept, lines[0]).T if len(lines) == 1 else contract(jnp.concatenate(lines, axis=0), kept)
        for i, source in enumerate(sources):
            here = value[i * 2 * rows : (i + 1) * 2 * rows].reshape(2, 2, share, 2 * count)
            part[:, pl.ds(source * 2, 2), :, own_pair] = here

    def send_parts(g, columns):
        for i, s in enumerate(shifts):
            chunk, to = plane(*s)
            go(
                remote(
                    part.at[g, chunk, :, columns], parts.at[g, i, :, columns], send_sem.at[PART], part_recv.at[g], to
                )
            )

    for t in range(4):
        for k in (0, 1):
            for h in (0, 1):
                for d in (UP, DOWN):
                    if t < STEPS[h][d]:
                        with scope(f"ag{t}{k}{h}{d}"):
                            ring_copy(k, h, d, t).wait_recv()
                        if t + 1 < STEPS[h][d]:
                            go(ring_copy(k, h, d, t + 1))
        if t == 1:
            pass_piece(0)
            with scope("tomate"):
                to_mate.wait_recv()
            with scope("S1"):
                own_parts([(z + Z + i) % Z for i in range(-2, 3)])
        if t == 2:
            pass_piece(1)
            with scope("S2"):
                own_parts([(z + Z - 3) % Z, (z + 3) % Z])
            pass_piece(2)
    with scope("S3"):
        own_parts([(z + 4) % Z])
    every = 2 * Z * rows

    def far_parts(first, size):
        return contract(
            bands[:, :, :, first : first + size].reshape(every, size),
            proj[1 - y_lo, :, :, first : first + size].reshape(2 * count, size),
        ).reshape(2, PLANE, share, 2 * count)

    for i in range(3):
        take_piece(i)
    with scope("Sfar0"):
        part[:, :, :, far_pair] = far_parts(0, cuts[3][0])
    pass_piece(3)
    take_piece(3)
    with scope("Sfar1"):
        part[:, :, :, far_pair] += far_parts(*cuts[3])
    pass_piece(4)
    with scope("mixes"):
        for copy in coef_copies:
            copy.wait_recv()
        down = lax.broadcasted_iota(jnp.int32, flat, 0)
        for s in range(4):
            for d in range(2 * per_atom - 1):
                mix[s, d] = jnp.sum(
                    jnp.where(down == inner + d - (per_atom - 1), coefs[s], 0.0), axis=0, keepdims=True
                )
    take_piece(4)
    with scope("Sfar2"):
        part[:, :, :, far_pair] += far_parts(*cuts[4])
    for g in (0, 1):
        send_parts(g, slice(None))
    for g in (0, 1):
        with scope(f"part{g}"):
            got_all(parts.at[g], part_recv.at[g])
        with scope(f"mix{g}"):
            total = part[g, me]
            for i in range(len(shifts)):
                total += parts[g, i]
            mixed = []
            for s in range(4):
                slot_total = total[:, s * count : (s + 1) * count]
                value = slot_total * mix[s, per_atom - 1]
                for d in range(2 * per_atom - 1):
                    if d != per_atom - 1:
                        value += pltpu.roll(slot_total, (count + per_atom - 1 - d) % count, 1) * mix[s, d]
                mixed.append(value)
            weighted[g, me] = jnp.concatenate(mixed, axis=1).astype(BF16)
        for i, s in enumerate(shifts):
            _, to = plane(*s)
            there = weighted.at[g, me]
            go(remote(there, there, send_sem.at[WEIGHTED], wt_recv.at[g], to))

    group = Z * rows
    tile = 512
    width = half // PARTS
    spans = [slice(h * width, (h + 1) * width) for h in range(PARTS)]

    def own_sum(g, h, owner):
        return result[g, owner, :, spans[h]]

    def at_step(h, d, t):
        return d * STEPS[h][UP] + t

    def sum_copy(g, h, d, t):
        n = at_step(h, d, t)
        if t < STEPS[h][d] - 1:
            return remote(
                sent.at[g, h, n], came.at[g, h, n], send_sem.at[SUM], sum_recv.at[g, h, n - d], z_next[d]
            )
        owner = at(g, (z + 1) % Z if d == UP else (z + Z - 1) % Z, core)
        return remote(sent.at[g, h, n], last.at[y_lo, h, d], send_sem.at[SUM], last_recv.at[y_lo, h], owner)

    def arrived(g, h, d, t):
        return came[g, h, at_step(h, d, t)].astype(F32)

    def sum_step(g, h, d, t):
        n = STEPS[h][d]
        owner = (z + (n - t)) % Z if d == UP else (z + Z - (n - t)) % Z
        value = own_sum(g, h, owner)
        if t > 0:
            with scope(f"rs{t - 1}{h}{d}"):
                sum_copy(g, h, d, t - 1).wait_recv()
            value += arrived(g, h, d, t - 1)
        sent[g, h, at_step(h, d, t)] = value.astype(BF16)
        go(sum_copy(g, h, d, t))

    for g in (0, 1):
        with scope(f"wt{g}"):
            got_all(weighted.at[g, pl.ds(0, PLANE - 1)], wt_recv.at[g])
        for h in range(PARTS):
            with scope(f"O{g}{h}"):
                for first in range(spans[h].start, spans[h].stop, tile):
                    size = min(tile, spans[h].stop - first)
                    value = jnp.dot(
                        weighted[g].reshape(group, 4 * count),
                        proj[:, :, :, first : first + size].reshape(4 * count, size),
                        preferred_element_type=F32,
                    )
                    result[g, :, :, first : first + size] = value.reshape(Z, rows, size)
            for d in (UP, DOWN):
                sum_step(g, h, d, 0)
    final[1 - y_lo] = result[1 - y_lo, z].astype(BF16)
    own_share = go(remote(final.at[1 - y_lo], across_share, send_sem.at[END], end_recv.at[0], across))
    order = [(g, h, t) for t in (1, 2, 3) for g in (0, 1) for h in range(PARTS)]
    for g, h, t in order:
        for d in (UP, DOWN):
            if t < STEPS[h][d]:
                sum_step(g, h, d, t)
    with scope("share"):
        own_share.wait_recv()
        sent_all(final.at[0], send_sem.at[END])
    for h in range(PARTS):
        for side, value in ((y_lo, result[y_lo, z, :, spans[h]]), (1 - y_lo, across_share[:, spans[h]].astype(F32))):
            with scope(f"last{h}"):
                got_all(last.at[side, h], last_recv.at[side, h])
            for d in (UP, DOWN):
                value += last[side, h, d].astype(F32)
            out_ref[:, columns_of(side, h * width, width)] = value.astype(BF16)
    with scope("drain"):
        sent_all(bands.at[:, pl.ds(0, Z - 1)], send_sem.at[RING])
        sent_all(away, send_sem.at[ACROSS])
        sent_all(proj.at[0, 0], send_sem.at[MATE])
        sent_all(coefs.at[pl.ds(0, 3)], send_sem.at[COEFS])

        @pl.when(core == 0)
        def _():
            sent_all(stage, send_sem.at[HAND])

        @pl.when(core == 1)
        def _():
            sent_all(proj.at[0], send_sem.at[PIECE_SEND])
            sent_all(proj.at[0], send_sem.at[PASS])

        sent_all(parts, send_sem.at[PART])
        sent_all(weighted.at[:, pl.ds(0, PLANE - 1)], send_sem.at[WEIGHTED])
        sent_all(bands.at[:, pl.ds(0, Z - 1)], send_sem.at[SUM])


def shards(wave_rows, projectors, dij_table, dij_index, proj_count):
    rows, width = wave_rows.shape
    count = projectors.shape[0]
    half = width // 2
    kinds, per_atom, _ = dij_table.shape
    atoms = count // per_atom

    dma = pltpu.SemaphoreType.DMA
    others = PLANE - 1
    hbm = pl.BlockSpec(memory_space=pltpu.MemorySpace.HBM)
    operands = [
        pltpu.with_memory_space_constraint(value, pltpu.MemorySpace.HBM)
        for value in (wave_rows, projectors, jnp.transpose(dij_table, (1, 2, 0)), dij_index, proj_count)
    ]
    return pl.pallas_call(
        kernel,
        out_shape=jax.ShapeDtypeStruct((rows, width), BF16),
        in_specs=[hbm] * 5,
        out_specs=pl.BlockSpec(memory_space=pltpu.MemorySpace.VMEM),
        scratch_shapes=[
            pltpu.VMEM((2, Z, rows, half), BF16),
            pltpu.VMEM((rows, half), BF16),
            pltpu.VMEM((count, half), BF16),
            pltpu.VMEM((2, 2, count, half), BF16),
            pltpu.VMEM((per_atom, per_atom, kinds), F32),
            pltpu.SMEM((atoms,), jnp.int32),
            pltpu.SMEM((atoms,), jnp.int32),
            pltpu.VMEM((4, per_atom, count), F32),
            pltpu.VMEM((2, PLANE, rows // 2, 4 * count), F32),
            pltpu.VMEM((2, others, rows // 2, 4 * count), F32),
            pltpu.VMEM((2, PLANE, rows // 2, 4 * count), BF16),
            pltpu.VMEM((2, Z, rows, half), F32),
            pltpu.VMEM((2, PARTS, Z - 1, rows, half // PARTS), BF16),
            pltpu.VMEM((2, PARTS, Z - 1, rows, half // PARTS), BF16),
            pltpu.VMEM((2, PARTS, 2, rows, half // PARTS), BF16),
            pltpu.VMEM((rows, half), BF16),
            pltpu.VMEM((2, rows, half), BF16),
            pltpu.VMEM((4, 2 * per_atom - 1, 1, count), F32),
            dma((SENDS,)),
            dma((2, 2, Z - 1)),
            dma((2,)),
            dma((1,)),
            dma((3,)),
            dma((1,)),
            dma((2, len(PIECES))),
            dma((len(PIECES),)),
            dma((2,)),
            dma((2,)),
            dma((2, PARTS, Z - 3)),
            dma((2, PARTS)),
            dma((1,)),
            dma((2 * PARTS,)),
        ],
        compiler_params=pltpu.CompilerParams(
            collective_id=0, has_side_effects=True, vmem_limit_bytes=40 * 1024 * 1024
        ),
        name="nonlocal_rows",
    )(*operands)


def solution(mesh):
    return jax.shard_map(
        shards,
        mesh=mesh,
        in_specs=(P("atom", "band"), P("atom", "band"), P(), P("atom"), P("atom")),
        out_specs=P("atom", "band"),
        check_vma=False,
    )
```

```python
import functools

import jax
import jax.numpy as jnp
from jax import lax
from jax.experimental import pallas as pl
from jax.experimental.pallas import tpu as pltpu
from jax.sharding import PartitionSpec as P

MESH = pl.DeviceIdType.MESH
F32 = jnp.float32
BF16 = jnp.bfloat16
scope = jax.named_scope
Z = 8
SIDE = 4
PLANE = SIDE * SIDE
PARTS = 2
PIECES = (1024, 1024, 1024, 896, 128)
UP, DOWN = 0, 1
RING, ACROSS, HAND, PIECE_SEND, MATE, COEFS, PASS, PART, WEIGHTED, SUM, END = range(11)
SENDS = 11
STEPS = ((4, 3), (3, 4), (4, 3), (3, 4))


def kernel(
    wave_ref, proj_ref, table_ref, index_ref, count_ref, out_ref,
    bands, away, stage, proj, table, index, acting, coefs, part, parts, weighted, result, sent, came, last, across_share, final, mix,
    send_sem, ring_recv, y_recv, mate_recv, c_recv, hand_recv, piece_recv, pass_recv, part_recv, wt_recv, sum_recv, last_recv, end_recv,
    local_sem,
):
    rows, half = away.shape
    count = proj.shape[2]
    per_atom, _, kinds = table.shape
    share = rows // 2
    atom, band = lax.axis_index("atom"), lax.axis_index("band")
    y_lo, z, core = atom // (2 * Z), (atom // 2) % Z, atom % 2
    y_hi, x = band // SIDE, band % SIDE
    y = y_hi * 2 + y_lo
    me = y * SIDE + x
    slot = y_lo * 2 + core

    def at(lo, zz, cc, hi=y_hi, xx=x):
        return (lo * (2 * Z) + zz * 2 + cc, hi * SIDE + xx)

    mate = at(y_lo, z, 1 - core)
    across = at(1 - y_lo, z, core)
    corner = at(1 - y_lo, z, 1 - core)
    z_next = (at(y_lo, (z + 1) % Z, core), at(y_lo, (z + Z - 1) % Z, core))
    shifts = [(dy, dx) for dy in range(SIDE) for dx in range(SIDE) if dy or dx]
    shifts.sort(key=lambda s: -2 * min(s[0], SIDE - s[0]) - min(s[1], SIDE - s[1]))

    def plane(dy, dx):
        yy, xx = (y + dy) % SIDE, (x + dx) % SIDE
        return yy * SIDE + xx, at(yy % 2, z, core, yy // 2, xx)

    def remote(src, dst, send, recv, to):
        return pltpu.make_async_remote_copy(
            src_ref=src, dst_ref=dst, send_sem=send, recv_sem=recv, device_id=to, device_id_type=MESH
        )

    def columns_of(side, first, size):
        return pl.ds(pl.multiple_of(side * half + first, 128), size)

    mine, theirs = columns_of(y_lo, 0, half), columns_of(1 - y_lo, 0, half)
    away_bands = pltpu.make_async_copy(wave_ref.at[:, theirs], away, local_sem.at[0])
    own_bands = pltpu.make_async_copy(wave_ref.at[:, mine], bands.at[y_lo, z], local_sem.at[1])
    own_proj = pltpu.make_async_copy(proj_ref.at[:, mine], proj.at[y_lo, core], local_sem.at[2])
    small = [
        pltpu.make_async_copy(table_ref, table, local_sem.at[3]),
        pltpu.make_async_copy(index_ref, index, local_sem.at[4]),
        pltpu.make_async_copy(count_ref, acting, local_sem.at[5]),
    ]
    for copy in (away_bands, own_bands, own_proj, *small):
        copy.start()

    barrier = pltpu.get_barrier_semaphore()
    slant = (at(1 - y_lo, (z + 1) % Z, core), at(1 - y_lo, (z + Z - 1) % Z, core))
    greet = [mate, corner, *z_next, *slant] + [plane(*s)[1] for s in shifts]
    for to in greet:
        pl.semaphore_signal(barrier, inc=1, device_id=to, device_id_type=MESH)
    with scope("barrier"):
        pl.semaphore_wait(barrier, len(greet))

    def go(copy):
        copy.start()
        return copy

    def sent_all(ref, sem):
        remote(ref, ref, sem, sem, mate).wait_send()

    def got_all(ref, sem):
        remote(ref, ref, sem, sem, mate).wait_recv()

    def ring_copy(k, h, d, t):
        source = (z + Z - t) % Z if d == UP else (z + t) % Z
        block = bands.at[y_lo if k == 0 else 1 - y_lo, source, :, pl.ds(h * (half // 2), half // 2)]
        return remote(block, block, send_sem.at[RING], ring_recv.at[k, h, d * STEPS[h][UP] + t], z_next[d])

    away_bands.wait()
    y_bands = []
    for h in (0, 1):
        columns = pl.ds(h * (half // 2), half // 2)
        y_bands.append(
            go(remote(away.at[:, columns], bands.at[y_lo, z, :, columns], send_sem.at[ACROSS], y_recv.at[h], across))
        )
    own_bands.wait()
    for h in (0, 1):
        for d in (UP, DOWN):
            go(ring_copy(0, h, d, 0))
    cuts = [(sum(PIECES[:i]), size) for i, size in enumerate(PIECES)]
    hand = remote(proj_ref.at[:, theirs], stage, send_sem.at[HAND], hand_recv.at[0], mate)
    pieces = [
        [
            remote(
                source, proj.at[y_lo, c, :, pl.ds(first, size)], send_sem.at[PIECE_SEND], piece_recv.at[c, i], across
            )
            for c, source in (
                (0, stage.at[:, pl.ds(first, size)]), (1, proj_ref.at[:, columns_of(1 - y_lo, first, size)])
            )
        ]
        for i, (first, size) in enumerate(cuts)
    ]

    @pl.when(core == 0)
    def _():
        hand.start()

    @pl.when(core == 1)
    def _():
        for i in (0, 1):
            pieces[i][1].start()

    own_proj.wait()
    there = proj.at[y_lo, core]
    to_mate = go(remote(there, there, send_sem.at[MATE], mate_recv.at[0], mate))

    for copy in small:
        copy.wait()
    flat = (per_atom, count)
    lane = lax.broadcasted_iota(jnp.int32, flat, 1)
    inner = lane % per_atom
    chosen = jnp.zeros(flat, jnp.int32)
    limit = jnp.zeros(flat, jnp.int32)
    for a in range(count // per_atom):
        chosen = jnp.where(lane // per_atom == a, index[a], chosen)
        limit = jnp.where(lane // per_atom == a, acting[a], limit)
    kind = lax.broadcasted_iota(jnp.int32, (kinds, count), 0)
    value = jnp.zeros(flat, F32)
    for i in range(per_atom):
        pick = jnp.where((kind == chosen[:1]) & (inner[:1] == i), 1.0, 0.0).astype(F32)
        value += jnp.dot(table[i], pick, precision=lax.Precision.HIGHEST, preferred_element_type=F32)
    on = (inner < limit) & (lax.broadcasted_iota(jnp.int32, flat, 0) < limit)
    coefs[slot] = jnp.where(on, value, 0.0)

    coef_copies = [
        go(remote(coefs.at[slot], coefs.at[slot], send_sem.at[COEFS], c_recv.at[i], to))
        for i, to in enumerate((mate, across, corner))
    ]
    for h in (0, 1):
        with scope(f"ybands{h}"):
            y_bands[h].wait_recv()
        for d in (UP, DOWN):
            go(ring_copy(1, h, d, 0))

    @pl.when(core == 1)
    def _():
        hand.wait_recv()
        for i in (0, 1):
            pieces[i][0].start()
        for pair in pieces[2:]:
            for copy in pair:
                copy.start()

    def passing(i):
        first, size = cuts[i]
        there = proj.at[1 - y_lo, :, :, pl.ds(first, size)]
        return remote(there, there, send_sem.at[PASS], pass_recv.at[i], mate)

    def pass_piece(i):
        @pl.when(core == 1)
        def _():
            with scope(f"piece{i}"):
                for copy in pieces[i]:
                    copy.wait_recv()
            passing(i).start()

    def take_piece(i):
        @pl.when(core == 0)
        def _():
            with scope(f"take{i}"):
                passing(i).wait_recv()

    def contract(lines, kept):
        return lax.dot_general(lines, kept, (((1,), (1,)), ((), ())), preferred_element_type=F32)

    own_pair = pl.ds(pl.multiple_of(y_lo * 2 * count, count), 2 * count)
    far_pair = pl.ds(pl.multiple_of((1 - y_lo) * 2 * count, count), 2 * count)

    def own_parts(sources):
        lines = [bands[:, source].reshape(2 * rows, half) for source in sources]
        kept = proj[y_lo].reshape(2 * count, half)
        value = contract(kept, lines[0]).T if len(lines) == 1 else contract(jnp.concatenate(lines, axis=0), kept)
        for i, source in enumerate(sources):
            here = value[i * 2 * rows : (i + 1) * 2 * rows].reshape(2, 2, share, 2 * count)
            part[:, pl.ds(source * 2, 2), :, own_pair] = here

    def send_parts(g, columns):
        for i, s in enumerate(shifts):
            chunk, to = plane(*s)
            go(
                remote(
                    part.at[g, chunk, :, columns], parts.at[g, i, :, columns], send_sem.at[PART], part_recv.at[g], to
                )
            )

    for t in range(4):
        for k in (0, 1):
            for h in (0, 1):
                for d in (UP, DOWN):
                    if t < STEPS[h][d]:
                        with scope(f"ag{t}{k}{h}{d}"):
                            ring_copy(k, h, d, t).wait_recv()
                        if t + 1 < STEPS[h][d]:
                            go(ring_copy(k, h, d, t + 1))
        if t == 1:
            pass_piece(0)
            with scope("tomate"):
                to_mate.wait_recv()
            with scope("S1"):
                own_parts([(z + Z + i) % Z for i in range(-2, 3)])
        if t == 2:
            pass_piece(1)
            with scope("S2"):
                own_parts([(z + Z - 3) % Z, (z + 3) % Z])
            pass_piece(2)
    with scope("S3"):
        own_parts([(z + 4) % Z])
    every = 2 * Z * rows

    def far_parts(first, size):
        return contract(
            bands[:, :, :, first : first + size].reshape(every, size),
            proj[1 - y_lo, :, :, first : first + size].reshape(2 * count, size),
        ).reshape(2, PLANE, share, 2 * count)

    for i in range(3):
        take_piece(i)
    with scope("Sfar0"):
        part[:, :, :, far_pair] = far_parts(0, cuts[3][0])
    pass_piece(3)
    take_piece(3)
    with scope("Sfar1"):
        part[:, :, :, far_pair] += far_parts(*cuts[3])
    pass_piece(4)
    with scope("mixes"):
        for copy in coef_copies:
            copy.wait_recv()
        down = lax.broadcasted_iota(jnp.int32, flat, 0)
        for s in range(4):
            for d in range(2 * per_atom - 1):
                mix[s, d] = jnp.sum(
                    jnp.where(down == inner + d - (per_atom - 1), coefs[s], 0.0), axis=0, keepdims=True
                )
    take_piece(4)
    with scope("Sfar2"):
        part[:, :, :, far_pair] += far_parts(*cuts[4])
    for g in (0, 1):
        send_parts(g, slice(None))
    for g in (0, 1):
        with scope(f"part{g}"):
            got_all(parts.at[g], part_recv.at[g])
        with scope(f"mix{g}"):
            total = part[g, me]
            for i in range(len(shifts)):
                total += parts[g, i]
            mixed = []
            for s in range(4):
                slot_total = total[:, s * count : (s + 1) * count]
                value = slot_total * mix[s, per_atom - 1]
                for d in range(2 * per_atom - 1):
                    if d != per_atom - 1:
                        value += pltpu.roll(slot_total, (count + per_atom - 1 - d) % count, 1) * mix[s, d]
                mixed.append(value)
            weighted[g, me] = jnp.concatenate(mixed, axis=1).astype(BF16)
        for i, s in enumerate(shifts):
            _, to = plane(*s)
            there = weighted.at[g, me]
            go(remote(there, there, send_sem.at[WEIGHTED], wt_recv.at[g], to))

    group = Z * rows
    tile = 512
    width = half // PARTS
    spans = [slice(h * width, (h + 1) * width) for h in range(PARTS)]

    def own_sum(g, h, owner):
        return result[g, owner, :, spans[h]]

    def at_step(h, d, t):
        return d * STEPS[h][UP] + t

    def sum_copy(g, h, d, t):
        n = at_step(h, d, t)
        if t < STEPS[h][d] - 1:
            return remote(
                sent.at[g, h, n], came.at[g, h, n], send_sem.at[SUM], sum_recv.at[g, h, n - d], z_next[d]
            )
        owner = at(g, (z + 1) % Z if d == UP else (z + Z - 1) % Z, core)
        return remote(sent.at[g, h, n], last.at[y_lo, h, d], send_sem.at[SUM], last_recv.at[y_lo, h], owner)

    def arrived(g, h, d, t):
        return came[g, h, at_step(h, d, t)].astype(F32)

    def sum_step(g, h, d, t):
        n = STEPS[h][d]
        owner = (z + (n - t)) % Z if d == UP else (z + Z - (n - t)) % Z
        value = own_sum(g, h, owner)
        if t > 0:
            with scope(f"rs{t - 1}{h}{d}"):
                sum_copy(g, h, d, t - 1).wait_recv()
            value += arrived(g, h, d, t - 1)
        sent[g, h, at_step(h, d, t)] = value.astype(BF16)
        go(sum_copy(g, h, d, t))

    for g in (0, 1):
        with scope(f"wt{g}"):
            got_all(weighted.at[g, pl.ds(0, PLANE - 1)], wt_recv.at[g])
        for h in range(PARTS):
            with scope(f"O{g}{h}"):
                for first in range(spans[h].start, spans[h].stop, tile):
                    size = min(tile, spans[h].stop - first)
                    value = jnp.dot(
                        weighted[g].reshape(group, 4 * count),
                        proj[:, :, :, first : first + size].reshape(4 * count, size),
                        preferred_element_type=F32,
                    )
                    result[g, :, :, first : first + size] = value.reshape(Z, rows, size)
            for d in (UP, DOWN):
                sum_step(g, h, d, 0)
    final[1 - y_lo] = result[1 - y_lo, z].astype(BF16)
    own_share = go(remote(final.at[1 - y_lo], across_share, send_sem.at[END], end_recv.at[0], across))
    order = [(g, h, t) for t in (1, 2, 3) for g in (0, 1) for h in range(PARTS)]
    for g, h, t in order:
        for d in (UP, DOWN):
            if t < STEPS[h][d]:
                sum_step(g, h, d, t)
    with scope("share"):
        own_share.wait_recv()
        sent_all(final.at[0], send_sem.at[END])
    for h in range(PARTS):
        for side, value in ((y_lo, result[y_lo, z, :, spans[h]]), (1 - y_lo, across_share[:, spans[h]].astype(F32))):
            with scope(f"last{h}"):
                got_all(last.at[side, h], last_recv.at[side, h])
            for d in (UP, DOWN):
                value += last[side, h, d].astype(F32)
            out_ref[:, columns_of(side, h * width, width)] = value.astype(BF16)
    with scope("drain"):
        sent_all(bands.at[:, pl.ds(0, Z - 1)], send_sem.at[RING])
        sent_all(away, send_sem.at[ACROSS])
        sent_all(proj.at[0, 0], send_sem.at[MATE])
        sent_all(coefs.at[pl.ds(0, 3)], send_sem.at[COEFS])

        @pl.when(core == 0)
        def _():
            sent_all(stage, send_sem.at[HAND])

        @pl.when(core == 1)
        def _():
            sent_all(proj.at[0], send_sem.at[PIECE_SEND])
            sent_all(proj.at[0], send_sem.at[PASS])

        sent_all(parts, send_sem.at[PART])
        sent_all(weighted.at[:, pl.ds(0, PLANE - 1)], send_sem.at[WEIGHTED])
        sent_all(bands.at[:, pl.ds(0, Z - 1)], send_sem.at[SUM])


def shards(wave_rows, projectors, dij_table, dij_index, proj_count):
    rows, width = wave_rows.shape
    count = projectors.shape[0]
    half = width // 2
    kinds, per_atom, _ = dij_table.shape
    atoms = count // per_atom

    dma = pltpu.SemaphoreType.DMA
    others = PLANE - 1
    hbm = pl.BlockSpec(memory_space=pltpu.MemorySpace.HBM)
    operands = [
        pltpu.with_memory_space_constraint(value, pltpu.MemorySpace.HBM)
        for value in (wave_rows, projectors, jnp.transpose(dij_table, (1, 2, 0)), dij_index, proj_count)
    ]
    return pl.pallas_call(
        kernel,
        out_shape=jax.ShapeDtypeStruct((rows, width), BF16),
        in_specs=[hbm] * 5,
        out_specs=pl.BlockSpec(memory_space=pltpu.MemorySpace.VMEM),
        scratch_shapes=[
            pltpu.VMEM((2, Z, rows, half), BF16),
            pltpu.VMEM((rows, half), BF16),
            pltpu.VMEM((count, half), BF16),
            pltpu.VMEM((2, 2, count, half), BF16),
            pltpu.VMEM((per_atom, per_atom, kinds), F32),
            pltpu.SMEM((atoms,), jnp.int32),
            pltpu.SMEM((atoms,), jnp.int32),
            pltpu.VMEM((4, per_atom, count), F32),
            pltpu.VMEM((2, PLANE, rows // 2, 4 * count), F32),
            pltpu.VMEM((2, others, rows // 2, 4 * count), F32),
            pltpu.VMEM((2, PLANE, rows // 2, 4 * count), BF16),
            pltpu.VMEM((2, Z, rows, half), F32),
            pltpu.VMEM((2, PARTS, Z - 1, rows, half // PARTS), BF16),
            pltpu.VMEM((2, PARTS, Z - 1, rows, half // PARTS), BF16),
            pltpu.VMEM((2, PARTS, 2, rows, half // PARTS), BF16),
            pltpu.VMEM((rows, half), BF16),
            pltpu.VMEM((2, rows, half), BF16),
            pltpu.VMEM((4, 2 * per_atom - 1, 1, count), F32),
            dma((SENDS,)),
            dma((2, 2, Z - 1)),
            dma((2,)),
            dma((1,)),
            dma((3,)),
            dma((1,)),
            dma((2, len(PIECES))),
            dma((len(PIECES),)),
            dma((2,)),
            dma((2,)),
            dma((2, PARTS, Z - 3)),
            dma((2, PARTS)),
            dma((1,)),
            dma((6,)),
        ],
        compiler_params=pltpu.CompilerParams(
            collective_id=0, has_side_effects=True, vmem_limit_bytes=40 * 1024 * 1024
        ),
        name="nonlocal_rows",
    )(*operands)


def solution(mesh):
    return jax.shard_map(
        shards,
        mesh=mesh,
        in_specs=(P("atom", "band"), P("atom", "band"), P(), P("atom"), P("atom")),
        out_specs=P("atom", "band"),
        check_vma=False,
    )
```

```python
import functools

import jax
import jax.numpy as jnp
from jax import lax
from jax.experimental import pallas as pl
from jax.experimental.pallas import tpu as pltpu
from jax.sharding import PartitionSpec as P

MESH = pl.DeviceIdType.MESH
F32 = jnp.float32
BF16 = jnp.bfloat16
scope = jax.named_scope
Z = 8
SIDE = 4
PLANE = SIDE * SIDE
PARTS = 4
PIECES = (1024, 1024, 1024, 896, 128)
UP, DOWN = 0, 1
RING, ACROSS, HAND, PIECE_SEND, MATE, COEFS, PASS, PART, WEIGHTED, SUM, END = range(11)
SENDS = 11
STEPS = ((4, 3), (3, 4), (4, 3), (3, 4))


def kernel(
    wave_ref, proj_ref, table_ref, index_ref, count_ref, out_ref,
    bands, away, stage, proj, table, index, acting, coefs, part, parts, weighted, result, sent, came, last, across_share, final, mix,
    send_sem, ring_recv, y_recv, mate_recv, c_recv, hand_recv, piece_recv, pass_recv, part_recv, wt_recv, sum_recv, last_recv, end_recv,
    local_sem,
):
    rows, half = away.shape
    count = proj.shape[2]
    per_atom, _, kinds = table.shape
    share = rows // 2
    atom, band = lax.axis_index("atom"), lax.axis_index("band")
    y_lo, z, core = atom // (2 * Z), (atom // 2) % Z, atom % 2
    y_hi, x = band // SIDE, band % SIDE
    y = y_hi * 2 + y_lo
    me = y * SIDE + x
    slot = y_lo * 2 + core

    def at(lo, zz, cc, hi=y_hi, xx=x):
        return (lo * (2 * Z) + zz * 2 + cc, hi * SIDE + xx)

    mate = at(y_lo, z, 1 - core)
    across = at(1 - y_lo, z, core)
    corner = at(1 - y_lo, z, 1 - core)
    z_next = (at(y_lo, (z + 1) % Z, core), at(y_lo, (z + Z - 1) % Z, core))
    shifts = [(dy, dx) for dy in range(SIDE) for dx in range(SIDE) if dy or dx]
    shifts.sort(key=lambda s: -2 * min(s[0], SIDE - s[0]) - min(s[1], SIDE - s[1]))

    def plane(dy, dx):
        yy, xx = (y + dy) % SIDE, (x + dx) % SIDE
        return yy * SIDE + xx, at(yy % 2, z, core, yy // 2, xx)

    def remote(src, dst, send, recv, to):
        return pltpu.make_async_remote_copy(
            src_ref=src, dst_ref=dst, send_sem=send, recv_sem=recv, device_id=to, device_id_type=MESH
        )

    def columns_of(side, first, size):
        return pl.ds(pl.multiple_of(side * half + first, 128), size)

    mine, theirs = columns_of(y_lo, 0, half), columns_of(1 - y_lo, 0, half)
    away_bands = pltpu.make_async_copy(wave_ref.at[:, theirs], away, local_sem.at[0])
    own_bands = pltpu.make_async_copy(wave_ref.at[:, mine], bands.at[y_lo, z], local_sem.at[1])
    own_proj = pltpu.make_async_copy(proj_ref.at[:, mine], proj.at[y_lo, core], local_sem.at[2])
    small = [
        pltpu.make_async_copy(table_ref, table, local_sem.at[3]),
        pltpu.make_async_copy(index_ref, index, local_sem.at[4]),
        pltpu.make_async_copy(count_ref, acting, local_sem.at[5]),
    ]
    for copy in (away_bands, own_bands, own_proj, *small):
        copy.start()

    barrier = pltpu.get_barrier_semaphore()
    slant = (at(1 - y_lo, (z + 1) % Z, core), at(1 - y_lo, (z + Z - 1) % Z, core))
    greet = [mate, corner, *z_next, *slant] + [plane(*s)[1] for s in shifts]
    for to in greet:
        pl.semaphore_signal(barrier, inc=1, device_id=to, device_id_type=MESH)
    with scope("barrier"):
        pl.semaphore_wait(barrier, len(greet))

    def go(copy):
        copy.start()
        return copy

    def sent_all(ref, sem):
        remote(ref, ref, sem, sem, mate).wait_send()

    def got_all(ref, sem):
        remote(ref, ref, sem, sem, mate).wait_recv()

    def ring_copy(k, h, d, t):
        source = (z + Z - t) % Z if d == UP else (z + t) % Z
        block = bands.at[y_lo if k == 0 else 1 - y_lo, source, :, pl.ds(h * (half // 2), half // 2)]
        return remote(block, block, send_sem.at[RING], ring_recv.at[k, h, d * STEPS[h][UP] + t], z_next[d])

    away_bands.wait()
    y_bands = []
    for h in (0, 1):
        columns = pl.ds(h * (half // 2), half // 2)
        y_bands.append(
            go(remote(away.at[:, columns], bands.at[y_lo, z, :, columns], send_sem.at[ACROSS], y_recv.at[h], across))
        )
    own_bands.wait()
    for h in (0, 1):
        for d in (UP, DOWN):
            go(ring_copy(0, h, d, 0))
    cuts = [(sum(PIECES[:i]), size) for i, size in enumerate(PIECES)]
    hand = remote(proj_ref.at[:, theirs], stage, send_sem.at[HAND], hand_recv.at[0], mate)
    pieces = [
        [
            remote(
                source, proj.at[y_lo, c, :, pl.ds(first, size)], send_sem.at[PIECE_SEND], piece_recv.at[i], across
            )
            for c, source in (
                (0, stage.at[:, pl.ds(first, size)]), (1, proj_ref.at[:, columns_of(1 - y_lo, first, size)])
            )
        ]
        for i, (first, size) in enumerate(cuts)
    ]

    @pl.when(core == 0)
    def _():
        hand.start()

    @pl.when(core == 1)
    def _():
        for i in (0, 1):
            pieces[i][1].start()

    own_proj.wait()
    there = proj.at[y_lo, core]
    to_mate = go(remote(there, there, send_sem.at[MATE], mate_recv.at[0], mate))

    for copy in small:
        copy.wait()
    flat = (per_atom, count)
    lane = lax.broadcasted_iota(jnp.int32, flat, 1)
    inner = lane % per_atom
    chosen = jnp.zeros(flat, jnp.int32)
    limit = jnp.zeros(flat, jnp.int32)
    for a in range(count // per_atom):
        chosen = jnp.where(lane // per_atom == a, index[a], chosen)
        limit = jnp.where(lane // per_atom == a, acting[a], limit)
    kind = lax.broadcasted_iota(jnp.int32, (kinds, count), 0)
    value = jnp.zeros(flat, F32)
    for i in range(per_atom):
        pick = jnp.where((kind == chosen[:1]) & (inner[:1] == i), 1.0, 0.0).astype(F32)
        value += jnp.dot(table[i], pick, precision=lax.Precision.HIGHEST, preferred_element_type=F32)
    on = (inner < limit) & (lax.broadcasted_iota(jnp.int32, flat, 0) < limit)
    coefs[slot] = jnp.where(on, value, 0.0)

    for to in (mate, across, corner):
        go(remote(coefs.at[slot], coefs.at[slot], send_sem.at[COEFS], c_recv.at[0], to))
    for h in (0, 1):
        with scope(f"ybands{h}"):
            y_bands[h].wait_recv()
        for d in (UP, DOWN):
            go(ring_copy(1, h, d, 0))

    @pl.when(core == 1)
    def _():
        hand.wait_recv()
        for i in (0, 1):
            pieces[i][0].start()
        for pair in pieces[2:]:
            for copy in pair:
                copy.start()

    def passed_block(i):
        first, size = cuts[i]
        return proj.at[1 - y_lo, :, :, pl.ds(first, size)]

    def passing(i):
        there = passed_block(i)
        return remote(there, there, send_sem.at[PASS], pass_recv.at[i], mate)

    def pass_piece(i):
        @pl.when(core == 1)
        def _():
            with scope(f"piece{i}"):
                got_all(passed_block(i), piece_recv.at[i])
            passing(i).start()

    def take_piece(i):
        @pl.when(core == 0)
        def _():
            with scope(f"take{i}"):
                passing(i).wait_recv()

    def contract(lines, kept):
        return lax.dot_general(lines, kept, (((1,), (1,)), ((), ())), preferred_element_type=F32)

    own_pair = pl.ds(pl.multiple_of(y_lo * 2 * count, count), 2 * count)
    far_pair = pl.ds(pl.multiple_of((1 - y_lo) * 2 * count, count), 2 * count)

    def own_parts(sources):
        lines = [bands[:, source].reshape(2 * rows, half) for source in sources]
        kept = proj[y_lo].reshape(2 * count, half)
        value = contract(kept, lines[0]).T if len(lines) == 1 else contract(jnp.concatenate(lines, axis=0), kept)
        for i, source in enumerate(sources):
            here = value[i * 2 * rows : (i + 1) * 2 * rows].reshape(2, 2, share, 2 * count)
            part[:, pl.ds(source * 2, 2), :, own_pair] = here

    def send_parts(g, columns):
        for i, s in enumerate(shifts):
            chunk, to = plane(*s)
            go(
                remote(
                    part.at[g, chunk, :, columns], parts.at[g, i, :, columns], send_sem.at[PART], part_recv.at[g], to
                )
            )

    for t in range(4):
        for k in (0, 1):
            for h in (0, 1):
                for d in (UP, DOWN):
                    if t < STEPS[h][d]:
                        with scope(f"ag{t}{k}{h}{d}"):
                            ring_copy(k, h, d, t).wait_recv()
                        if t + 1 < STEPS[h][d]:
                            go(ring_copy(k, h, d, t + 1))
        if t == 1:
            pass_piece(0)
            with scope("tomate"):
                to_mate.wait_recv()
            with scope("S1"):
                own_parts([(z + Z + i) % Z for i in range(-2, 3)])
        if t == 2:
            pass_piece(1)
            with scope("S2"):
                own_parts([(z + Z - 3) % Z, (z + 3) % Z])
            pass_piece(2)
    with scope("S3"):
        own_parts([(z + 4) % Z])
    every = 2 * Z * rows

    def far_parts(first, size):
        return contract(
            bands[:, :, :, first : first + size].reshape(every, size),
            proj[1 - y_lo, :, :, first : first + size].reshape(2 * count, size),
        ).reshape(2, PLANE, share, 2 * count)

    for i in range(3):
        take_piece(i)
    with scope("Sfar0"):
        part[:, :, :, far_pair] = far_parts(0, cuts[3][0])
    pass_piece(3)
    take_piece(3)
    with scope("Sfar1"):
        part[:, :, :, far_pair] += far_parts(*cuts[3])
    pass_piece(4)
    with scope("mixes"):
        got_all(coefs.at[pl.ds(0, 3)], c_recv.at[0])
        down = lax.broadcasted_iota(jnp.int32, flat, 0)
        for s in range(4):
            for d in range(2 * per_atom - 1):
                mix[s, d] = jnp.sum(
                    jnp.where(down == inner + d - (per_atom - 1), coefs[s], 0.0), axis=0, keepdims=True
                )
    take_piece(4)
    with scope("Sfar2"):
        part[:, :, :, far_pair] += far_parts(*cuts[4])
    for g in (0, 1):
        send_parts(g, slice(None))
    for g in (0, 1):
        with scope(f"part{g}"):
            got_all(parts.at[g], part_recv.at[g])
        with scope(f"mix{g}"):
            total = part[g, me]
            for i in range(len(shifts)):
                total += parts[g, i]
            mixed = []
            for s in range(4):
                slot_total = total[:, s * count : (s + 1) * count]
                value = slot_total * mix[s, per_atom - 1]
                for d in range(2 * per_atom - 1):
                    if d != per_atom - 1:
                        value += pltpu.roll(slot_total, (count + per_atom - 1 - d) % count, 1) * mix[s, d]
                mixed.append(value)
            weighted[g, me] = jnp.concatenate(mixed, axis=1).astype(BF16)
        for i, s in enumerate(shifts):
            _, to = plane(*s)
            there = weighted.at[g, me]
            go(remote(there, there, send_sem.at[WEIGHTED], wt_recv.at[g], to))

    group = Z * rows
    tile = 512
    width = half // PARTS
    spans = [slice(h * width, (h + 1) * width) for h in range(PARTS)]

    def own_sum(g, h, owner):
        return result[g, owner, :, spans[h]]

    def at_step(h, d, t):
        return d * STEPS[h][UP] + t

    def sum_copy(g, h, d, t):
        n = at_step(h, d, t)
        if t < STEPS[h][d] - 1:
            return remote(
                sent.at[g, h, n], came.at[g, h, n], send_sem.at[SUM], sum_recv.at[g, h, n - d], z_next[d]
            )
        owner = at(g, (z + 1) % Z if d == UP else (z + Z - 1) % Z, core)
        return remote(sent.at[g, h, n], last.at[y_lo, h, d], send_sem.at[SUM], last_recv.at[y_lo, h], owner)

    def arrived(g, h, d, t):
        return came[g, h, at_step(h, d, t)].astype(F32)

    def sum_step(g, h, d, t):
        n = STEPS[h][d]
        owner = (z + (n - t)) % Z if d == UP else (z + Z - (n - t)) % Z
        value = own_sum(g, h, owner)
        if t > 0:
            with scope(f"rs{t - 1}{h}{d}"):
                sum_copy(g, h, d, t - 1).wait_recv()
            value += arrived(g, h, d, t - 1)
        sent[g, h, at_step(h, d, t)] = value.astype(BF16)
        go(sum_copy(g, h, d, t))

    for g in (0, 1):
        with scope(f"wt{g}"):
            got_all(weighted.at[g, pl.ds(0, PLANE - 1)], wt_recv.at[g])
        for h in range(PARTS):
            with scope(f"O{g}{h}"):
                for first in range(spans[h].start, spans[h].stop, tile):
                    size = min(tile, spans[h].stop - first)
                    value = jnp.dot(
                        weighted[g].reshape(group, 4 * count),
                        proj[:, :, :, first : first + size].reshape(4 * count, size),
                        preferred_element_type=F32,
                    )
                    result[g, :, :, first : first + size] = value.reshape(Z, rows, size)
            for d in (UP, DOWN):
                sum_step(g, h, d, 0)
    final[1 - y_lo] = result[1 - y_lo, z].astype(BF16)
    own_share = go(remote(final.at[1 - y_lo], across_share, send_sem.at[END], end_recv.at[0], across))
    order = [(g, h, t) for t in (1, 2, 3) for g in (0, 1) for h in range(PARTS)]
    for g, h, t in order:
        for d in (UP, DOWN):
            if t < STEPS[h][d]:
                sum_step(g, h, d, t)
    with scope("share"):
        own_share.wait_recv()
        sent_all(final.at[0], send_sem.at[END])
    for h in range(PARTS):
        for side, value in ((y_lo, result[y_lo, z, :, spans[h]]), (1 - y_lo, across_share[:, spans[h]].astype(F32))):
            with scope(f"last{h}"):
                got_all(last.at[side, h], last_recv.at[side, h])
            for d in (UP, DOWN):
                value += last[side, h, d].astype(F32)
            out_ref[:, columns_of(side, h * width, width)] = value.astype(BF16)
    with scope("drain"):
        sent_all(bands.at[:, pl.ds(0, Z - 1)], send_sem.at[RING])
        sent_all(away, send_sem.at[ACROSS])
        sent_all(proj.at[0, 0], send_sem.at[MATE])
        sent_all(coefs.at[pl.ds(0, 3)], send_sem.at[COEFS])

        @pl.when(core == 0)
        def _():
            sent_all(stage, send_sem.at[HAND])

        @pl.when(core == 1)
        def _():
            sent_all(proj.at[0], send_sem.at[PIECE_SEND])
            sent_all(proj.at[0], send_sem.at[PASS])

        sent_all(parts, send_sem.at[PART])
        sent_all(weighted.at[:, pl.ds(0, PLANE - 1)], send_sem.at[WEIGHTED])
        sent_all(bands.at[:, pl.ds(0, Z - 1)], send_sem.at[SUM])


def shards(wave_rows, projectors, dij_table, dij_index, proj_count):
    rows, width = wave_rows.shape
    count = projectors.shape[0]
    half = width // 2
    kinds, per_atom, _ = dij_table.shape
    atoms = count // per_atom

    dma = pltpu.SemaphoreType.DMA
    others = PLANE - 1
    hbm = pl.BlockSpec(memory_space=pltpu.MemorySpace.HBM)
    operands = [
        pltpu.with_memory_space_constraint(value, pltpu.MemorySpace.HBM)
        for value in (wave_rows, projectors, jnp.transpose(dij_table, (1, 2, 0)), dij_index, proj_count)
    ]
    return pl.pallas_call(
        kernel,
        out_shape=jax.ShapeDtypeStruct((rows, width), BF16),
        in_specs=[hbm] * 5,
        out_specs=pl.BlockSpec(memory_space=pltpu.MemorySpace.VMEM),
        scratch_shapes=[
            pltpu.VMEM((2, Z, rows, half), BF16),
            pltpu.VMEM((rows, half), BF16),
            pltpu.VMEM((count, half), BF16),
            pltpu.VMEM((2, 2, count, half), BF16),
            pltpu.VMEM((per_atom, per_atom, kinds), F32),
            pltpu.SMEM((atoms,), jnp.int32),
            pltpu.SMEM((atoms,), jnp.int32),
            pltpu.VMEM((4, per_atom, count), F32),
            pltpu.VMEM((2, PLANE, rows // 2, 4 * count), F32),
            pltpu.VMEM((2, others, rows // 2, 4 * count), F32),
            pltpu.VMEM((2, PLANE, rows // 2, 4 * count), BF16),
            pltpu.VMEM((2, Z, rows, half), F32),
            pltpu.VMEM((2, PARTS, Z - 1, rows, half // PARTS), BF16),
            pltpu.VMEM((2, PARTS, Z - 1, rows, half // PARTS), BF16),
            pltpu.VMEM((2, PARTS, 2, rows, half // PARTS), BF16),
            pltpu.VMEM((rows, half), BF16),
            pltpu.VMEM((2, rows, half), BF16),
            pltpu.VMEM((4, 2 * per_atom - 1, 1, count), F32),
            dma((SENDS,)),
            dma((2, 2, Z - 1)),
            dma((2,)),
            dma((1,)),
            dma((1,)),
            dma((1,)),
            dma((len(PIECES),)),
            dma((len(PIECES),)),
            dma((2,)),
            dma((2,)),
            dma((2, PARTS, Z - 3)),
            dma((2, PARTS)),
            dma((1,)),
            dma((6,)),
        ],
        compiler_params=pltpu.CompilerParams(
            collective_id=0, has_side_effects=True, vmem_limit_bytes=40 * 1024 * 1024
        ),
        name="nonlocal_rows",
    )(*operands)


def solution(mesh):
    return jax.shard_map(
        shards,
        mesh=mesh,
        in_specs=(P("atom", "band"), P("atom", "band"), P(), P("atom"), P("atom")),
        out_specs=P("atom", "band"),
        check_vma=False,
    )
```
